128 devices in a mesh: dp: 64 (over z_hi, x, y, core), mp: 2 (over z_lo).
Axes of the slice: x: 4, y: 4, z: 4 (z_hi: 2, z_lo: 2; z = z_hi * 2 + z_lo), core: 2. Of those that a mesh axis runs over, the one named last changes fastest.
Arguments:
- inputs: bfloat16 [8192, 1792], P('dp', 'mp'), may hold values from -6 to 6
- cotangent: bfloat16 [8192, 1792], P('dp', 'mp'), may hold values from -6 to 6
- gate_weight: bfloat16 [9472, 1792], P(('mp', 'dp')), may hold values from -0.125 to 0.125
- up_weight: bfloat16 [9472, 1792], P(('mp', 'dp')), may hold values from -0.125 to 0.125
- down_weight: bfloat16 [9472, 1792], P(('mp', 'dp')), may hold values from -0.0625 to 0.0625
Outputs:
- input_grad: bfloat16 [8192, 1792], P('dp', 'mp')
- gate_grad: bfloat16 [9472, 1792], P(('mp', 'dp'))
The draws below stay inside these ranges and needn't reach their ends.
All inputs are finite; a program needn't handle non-finite values.
Results may differ from the reference program's by a relative error of at most 0.009.
Values may be sent and summed in bfloat16 or wider, within the bound.
A program may use at most 320 MiB of HBM per device.

```python
import jax
import jax.numpy as jnp
from jax import lax

D = 1792
FF = 9472
TOKENS = 8192


def levels(stream_key, shape, cuts, least, high):
    def one(dim, blocks):
        steps = jax.random.uniform(jax.random.fold_in(jax.random.fold_in(stream_key, 6), dim), (blocks,), jnp.float32, least / len(cuts), high / len(cuts))
        return jnp.repeat(jnp.exp(steps), shape[dim] // blocks).reshape((-1,) + (1,) * (len(shape) - dim - 1))

    level = one(*cuts[0])
    for cut in cuts[1:]:
        level = level * one(*cut)
    return level


def centred(own_key, extent, spread, limit, shards=(), held_as=jnp.bfloat16):
    values = jax.random.normal(own_key, extent, jnp.float32) * spread
    if len(shards) > 0:
        values = levels(own_key, extent, shards, -0.22, 0.18) * values
    return jnp.clip(values, min=-limit, max=limit).astype(held_as)


def setup_inputs(seed: int = 0) -> dict:
    streams_of = jax.random.split(jax.random.key(seed), 6)
    return {
        "inputs": centred(streams_of[0], (TOKENS, D), 1.0, 6.0, ((0, 64), (1, 2))),
        "cotangent": centred(streams_of[1], (TOKENS, D), 1.0, 6.0, ((0, 64), (1, 2))),
        "gate_weight": centred(streams_of[2], (FF, D), D ** -0.5, 0.125, ((0, 128),)),
        "up_weight": centred(streams_of[3], (FF, D), D ** -0.5, 0.125, ((0, 128),)),
        "down_weight": centred(streams_of[4], (FF, D), FF ** -0.5, 0.0625, ((0, 128),)),
    }


def tdot(left, right):
    return lax.dot_general(left, right, (((0,), (0,)), ((), ())), preferred_element_type=jnp.float32)


def rdot(left, right):
    return lax.dot_general(left, right, (((1,), (1,)), ((), ())), preferred_element_type=jnp.float32)


def reference(inputs, cotangent, gate_weight, up_weight, down_weight):
    gate = rdot(inputs, gate_weight)
    up = rdot(inputs, up_weight)
    sig = jax.nn.sigmoid(gate)
    act = gate * sig
    dhidden = rdot(cotangent, down_weight)
    dup = (dhidden * act).astype(jnp.bfloat16)
    dgate = (dhidden * up * sig * (1.0 + gate * (1.0 - sig))).astype(jnp.bfloat16)
    gate_grad = tdot(dgate, inputs).astype(jnp.bfloat16)
    input_grad = jnp.dot(dgate, gate_weight, preferred_element_type=jnp.float32)
    input_grad = input_grad + jnp.dot(dup, up_weight, preferred_element_type=jnp.float32)
    return input_grad.astype(jnp.bfloat16), gate_grad
```

```python
import jax
import jax.numpy as jnp
from jax import lax
from jax.sharding import Mesh
from jax.sharding import PartitionSpec as P

DP = ("dp_0", "dp_1", "dp_2", "dp_3")
MP_DP = ("mp", "dp_0", "dp_1", "dp_2", "dp_3")
TOK = ("dp_0", "dp_1", "mp")
HID = ("dp_2", "dp_3")


def tdot(left, right):
    return lax.dot_general(
        left, right, (((0,), (0,)), ((), ())), preferred_element_type=jnp.float32
    )


def rdot(left, right):
    return lax.dot_general(
        left, right, (((1,), (1,)), ((), ())), preferred_element_type=jnp.float32
    )


def whole_rows(pieces):
    groups, rows, width = pieces.shape
    halves = pieces.reshape(groups // 2, 2, rows, width)
    return jnp.moveaxis(halves, 1, 2).reshape(groups // 2 * rows, 2 * width)


def per_device(inputs, cotangent, gate_weight, up_weight, down_weight):
    rows, half = inputs.shape
    full_in = whole_rows(lax.all_gather(inputs, TOK, axis=0))
    full_cot = whole_rows(lax.all_gather(cotangent, TOK, axis=0))
    wg = lax.all_gather(gate_weight, HID, axis=0, tiled=True)
    wu = lax.all_gather(up_weight, HID, axis=0, tiled=True)
    wd = lax.all_gather(down_weight, HID, axis=0, tiled=True)
    gate = rdot(full_in, wg)
    up = rdot(full_in, wu)
    dhidden = rdot(full_cot, wd)
    sig = jax.nn.sigmoid(gate)
    act = gate * sig
    dup = (dhidden * act).astype(jnp.bfloat16)
    dgate = (dhidden * up * sig * (1.0 + gate * (1.0 - sig))).astype(jnp.bfloat16)
    total = jnp.dot(dgate, wg, preferred_element_type=jnp.float32)
    total = total + jnp.dot(dup, wu, preferred_element_type=jnp.float32)
    blocks = total.astype(jnp.bfloat16).reshape(-1, rows, 2, half)
    blocks = jnp.moveaxis(blocks, 2, 1).reshape(-1, rows, half)
    input_grad = lax.psum_scatter(blocks, TOK, scatter_dimension=0)
    gate_sum = tdot(dgate, full_in).astype(jnp.bfloat16)
    gate_grad = lax.psum_scatter(gate_sum, HID, scatter_dimension=0, tiled=True)
    return (input_grad, gate_grad)


def solution(mesh):
    torus = Mesh(
        mesh.devices.reshape(2, 4, 4, 2, mesh.shape["mp"]), ("dp_0", "dp_1", "dp_2", "dp_3", "mp")
    )
    return jax.shard_map(
        per_device,
        mesh=torus,
        in_specs=(P(DP, "mp"), P(DP, "mp"), P(MP_DP, None), P(MP_DP, None), P(MP_DP, None)),
        out_specs=(P(DP, "mp"), P(MP_DP, None)),
        check_vma=False,
    )
```

```python
import jax
import jax.numpy as jnp
from jax import lax
from jax.experimental import pallas as pl
from jax.experimental.pallas import tpu as pltpu
from jax.sharding import Mesh
from jax.sharding import PartitionSpec as P

DP = ("dp_0", "dp_1", "dp_2", "dp_3")
MP_DP = ("mp", "dp_0", "dp_1", "dp_2", "dp_3")
MESH = pl.DeviceIdType.MESH
F32 = jnp.float32
BF16 = jnp.bfloat16
N = 4
COPIES = 160


def dot(left, right, contract):
    return lax.dot_general(
        left, right, ((contract[:1], contract[1:]), ((), ())), preferred_element_type=F32
    )


class Links:
    def __init__(self, send, recv):
        self.send, self.recv, self.started = send, recv, []

    def copy(self, src, dst, device):
        k = len(self.started)
        c = pltpu.make_async_remote_copy(
            src_ref=src,
            dst_ref=dst,
            send_sem=self.send.at[k],
            recv_sem=self.recv.at[k],
            device_id=device,
            device_id_type=MESH,
        )
        c.start()
        self.started.append(c)
        return c

    def drain(self):
        for c in self.started:
            c.wait_send()


class Place:
    def __init__(self):
        self.x = lax.axis_index("dp_1")
        self.y = lax.axis_index("dp_2")
        self.c = lax.axis_index("dp_3")
        self.z = lax.axis_index("dp_0") * 2 + lax.axis_index("mp")

    def at_z(self, dz):
        z = lax.rem(self.z + (dz + N), N)
        return lax.div(z, 2), lax.rem(z, 2)

    def to(self, axis, step):
        if axis == "x":
            return {"dp_1": lax.rem(self.x + (step + N), N)}
        if axis == "y":
            return {"dp_2": lax.rem(self.y + (step + N), N)}
        if axis == "z":
            high, low = self.at_z(step)
            return {"dp_0": high, "mp": low}
        return {"dp_3": 1 - self.c}


class Tokens:
    def __init__(self, links, place, buf, own, p, q):
        self.links, self.place, self.buf, self.own = links, place, buf, own
        self.p, self.q = p, q
        self.rows, self.half = own.shape
        self.s2, self.f2 = {}, {}

    def slot(self, dx, dz, h):
        high, low = self.place.at_z(dz)
        rows = pl.ds(0, self.rows) if h is None else pl.ds(h * self.rows // 2, self.rows // 2)
        columns = pl.ds(pl.multiple_of(low * self.half, 128), self.half)
        return self.buf.at[dx % N, high, rows, columns]

    def piece(self, kp, kq):
        return (kp, kq) if self.p == "x" else (kq, kp)

    def push(self, kp, kq, h, axis, step):
        dx, dz = self.piece(kp, kq)
        src = self.own if (kp, kq) == (0, 0) else self.slot(dx, dz, h)
        ex = step if axis == "x" else 0
        return self.links.copy(src, self.slot(dx - ex, dz, h), self.place.to(axis, step))

    def start1(self):
        self.s1 = [self.push(0, 0, None, self.p, e) for e in (1, -1)]

    def both2(self, k, h):
        return [self.push(2 if k in ("lo", "hi") else k, 0, h, self.q, e) for e in (1, -1)]

    def start2(self):
        self.s2[0] = self.both2(0, None)

    def after1(self):
        self.s1[0].wait_recv()
        a = self.push(-1, 0, 0, self.p, 1)
        self.s1[1].wait_recv()
        b = self.push(1, 0, 1, self.p, -1)
        self.f1 = [a, b]
        self.s2[-1] = self.both2(-1, None)
        self.s2[1] = self.both2(1, None)

    def after_f1(self):
        self.f1[0].wait_recv()
        self.s2["lo"] = self.both2("lo", 0)
        self.f1[1].wait_recv()
        self.s2["hi"] = self.both2("hi", 1)

    def after2(self, k):
        self.s2[k][0].wait_recv()
        a = self.push(k, -1, 0, self.q, 1)
        self.s2[k][1].wait_recv()
        b = self.push(k, 1, 1, self.q, -1)
        self.f2[k] = [a, b]

    def after2_opposite(self):
        self.s2["lo"][0].wait_recv()
        a = self.push(2, -1, 0, self.q, 1)
        self.s2["hi"][1].wait_recv()
        b = self.push(2, 1, 1, self.q, -1)
        self.s2["lo"][1].wait_recv()
        self.s2["hi"][0].wait_recv()
        self.f2[2] = [a, b]

    def after_f2(self, k):
        for c in self.f2[k]:
            c.wait_recv()


class Weight:
    def __init__(self, links, place, buf, pad):
        self.links, self.place, self.buf, self.pad = links, place, buf, pad
        self.width = buf.shape[1]
        self.core = []

    def slot(self, c, dy, h):
        rows = pl.ds((c * N + dy % N) * self.pad, self.pad)
        if h is None:
            return self.buf.at[rows, :]
        return self.buf.at[rows, pl.ds(h * self.width // 2, self.width // 2)]

    def cross(self, dy, h):
        self.core.append(
            self.links.copy(self.slot(0, dy, h), self.slot(1, dy, h), self.place.to("c", 1))
        )

    def start(self):
        self.s = [
            self.links.copy(self.slot(0, 0, None), self.slot(0, -e, None), self.place.to("y", e))
            for e in (1, -1)
        ]
        self.cross(0, None)

    def after(self):
        self.s[0].wait_recv()
        a = self.links.copy(self.slot(0, -1, 0), self.slot(0, -2, 0), self.place.to("y", 1))
        self.s[1].wait_recv()
        b = self.links.copy(self.slot(0, 1, 1), self.slot(0, 2, 1), self.place.to("y", -1))
        self.f = [a, b]
        self.cross(-1, None)
        self.cross(1, None)

    def after_f(self):
        self.f[0].wait_recv()
        self.cross(2, 0)
        self.f[1].wait_recv()
        self.cross(2, 1)

    def finish(self):
        for c in self.core:
            c.wait_recv()


class Scatter:
    def __init__(self, links, place, axis, mine, send, recv):
        self.links, self.place, self.axis = links, place, axis
        self.mine, self.send, self.recv = mine, send, recv

    def go(self, value, u, h, step):
        self.send[u, h] = value.astype(BF16)
        return self.links.copy(
            self.send.at[u, h], self.recv.at[u, h], self.place.to(self.axis, step)
        )

    def first(self):
        self.a = self.go(self.mine(2, 0), 0, 0, 1)
        self.b = self.go(self.mine(2, 1), 0, 1, -1)

    def direct_right(self):
        self.r1 = self.go(self.mine(1, 1), 1, 1, 1)

    def direct_left(self):
        self.l0 = self.go(self.mine(-1, 0), 2, 0, -1)

    def second(self):
        self.a.wait_recv()
        self.r0 = self.go(self.mine(1, 0) + self.recv[0, 0].astype(F32), 1, 0, 1)
        self.b.wait_recv()
        self.l1 = self.go(self.mine(-1, 1) + self.recv[0, 1].astype(F32), 2, 1, -1)

    def total(self, h):
        (self.r1 if h else self.r0).wait_recv()
        (self.l1 if h else self.l0).wait_recv()
        return self.mine(0, h) + self.recv[1, h].astype(F32) + self.recv[2, h].astype(F32)


def kernel(
    x_ref, y_ref, g_ref, u_ref, d_ref, dx_out, dw_out,
    xb, yb, wb, gate, up, dgate, dup, dx, ra, rb, dwf, dwr,
    a1s, a1r, a2s, a2r, b1s, b1r, b2s, b2r, ws, wr, wcs,
    send_sem, recv_sem, own_sem,
):
    place = Place()
    links = Links(send_sem, recv_sem)
    rows, half = x_ref.shape
    units, width = g_ref.shape
    hidden = wb.shape[1]
    pad = hidden // (2 * N)
    quarter = rows // 4
    block = 2 * rows

    for m, ref in enumerate((g_ref, u_ref, d_ref)):
        if pad > units:
            low = units // 8 * 8
            wb[m, low:pad, :] = jnp.zeros((pad - low, width), BF16)
        wb[m, 0:units, :] = ref[...]
    barrier = pltpu.get_barrier_semaphore()
    peers = [("x", 1), ("x", -1), ("y", 1), ("y", -1), ("z", 1), ("z", -1), ("c", 1)]
    for axis, step in peers:
        pl.semaphore_signal(barrier, inc=1, device_id=place.to(axis, step), device_id_type=MESH)
    pl.semaphore_wait(barrier, len(peers))

    tx = Tokens(links, place, xb, x_ref, "z", "x")
    ty = Tokens(links, place, yb, y_ref, "x", "z")
    wg, wu, wd = (Weight(links, place, wb.at[m], pad) for m in range(3))
    tx.start1()
    ty.start1()
    wg.start()
    tx.start2()
    ty.start2()
    wu.start()
    keep = [
        pltpu.make_async_copy(x_ref, tx.slot(0, 0, None), own_sem.at[0]),
        pltpu.make_async_copy(y_ref, ty.slot(0, 0, None), own_sem.at[1]),
    ]
    for c in keep:
        c.start()
    for c in keep:
        c.wait()

    def tokens_of(buf, k):
        return buf[k % N].reshape(block, width)

    def columns(k):
        return slice(k % N * block, (k % N + 1) * block)

    def forward(out, m, k):
        out[:, columns(k)] = dot(wb[m], tokens_of(xb, k), (1, 1))

    def backward(k):
        dh = dot(wb[2], tokens_of(yb, k), (1, 1))
        g = gate[:, columns(k)]
        sig = jax.nn.sigmoid(g)
        dup[...] = (dh * (g * sig)).astype(BF16)
        dgate[:, columns(k)] = (
            dh * up[:, columns(k)] * sig * (1.0 + g * (1.0 - sig))
        ).astype(BF16)
        part = dot(dgate[:, columns(k)], wb[0], (0, 0)) + dot(dup[...], wb[1], (0, 0))
        dx[k % N] = part.reshape(2, rows, width)

    def z_part(ref, d, start, size):
        high, low = place.at_z(d)
        return ref[high, pl.ds(start, size), pl.ds(pl.multiple_of(low * half, 128), half)]

    a1 = Scatter(links, place, "x", lambda d, h: dx[d % N, h, 0 : rows // 2, :], a1s, a1r)
    a2 = Scatter(
        links, place, "z", lambda d, h: z_part(ra, d, h * quarter, quarter), a2s, a2r
    )
    b1 = [
        Scatter(
            links, place, "z",
            lambda d, h, k=k: z_part(dx.at[k], d, rows // 2 + h * quarter, quarter),
            b1s.at[k], b1r.at[k],
        )
        for k in range(N)
    ]
    b2 = Scatter(
        links, place, "x", lambda d, h: rb[d % N, h * quarter : (h + 1) * quarter, :], b2s, b2r
    )

    def dw_part(d, h):
        r = slice(d % N * pad, (d % N + 1) * pad)
        c = slice(h * half, (h + 1) * half)
        return dwf[r, c] + dwr[r, c].astype(F32)

    w1 = Scatter(links, place, "y", dw_part, ws, wr)

    def b1_start(k):
        b1[k % N].first()
        b1[k % N].direct_right()
        b1[k % N].direct_left()

    def b1_end(k):
        for h in range(2):
            rb[k % N, h * quarter : (h + 1) * quarter, :] = b1[k % N].total(h)

    tx.after1()
    ty.after1()
    wg.after()
    wd.start()
    tx.after2(0)
    ty.after2(0)
    wu.after()
    tx.after_f1()
    ty.after_f1()
    wg.after_f()
    wg.finish()
    forward(gate, 0, 0)
    tx.after2(-1)
    ty.after2(-1)
    wd.after()
    tx.after2(1)
    ty.after2(1)
    wu.after_f()
    wu.finish()
    forward(up, 1, 0)
    tx.after_f2(0)
    ty.after_f2(0)
    wd.after_f()
    wd.finish()
    tx.after2_opposite()
    ty.after2_opposite()
    backward(0)
    b1_start(0)
    for k in (-1, 1):
        forward(gate, 0, k)
        forward(up, 1, k)
        ty.after_f2(k)
        backward(k)
        b1_start(k)
        if k == 1:
            a1.direct_right()
        else:
            a1.direct_left()
    tx.after_f2(-1)
    tx.after_f2(1)
    tx.after_f2(2)
    forward(gate, 0, 2)
    forward(up, 1, 2)
    ty.after_f2(2)
    backward(2)
    a1.first()
    b1_start(2)

    b1[0].second()
    b1[N - 1].second()
    b1[1].second()
    whole = xb[...].reshape(N * block, width)
    other = hidden // 2
    wcs[...] = dot(dgate[other:, :], whole, (1, 0)).astype(BF16)
    cross = links.copy(wcs, dwr, place.to("c", 1))
    a1.second()
    b1[2].second()
    dwf[...] = dot(dgate[0:other, :], whole, (1, 0))
    b1_end(0)
    b1_end(-1)
    b1_end(1)
    cross.wait_recv()
    w1.first()
    w1.direct_right()
    w1.direct_left()
    b2.direct_right()
    b2.direct_left()
    for h in range(2):
        ra[h] = a1.total(h)
    a2.first()
    a2.direct_right()
    a2.direct_left()
    b1_end(2)
    b2.first()
    w1.second()
    a2.second()
    b2.second()
    for h in range(2):
        dw_out[:, h * half : (h + 1) * half] = w1.total(h)[0:units].astype(BF16)
    for h in range(2):
        dx_out[h * quarter : (h + 1) * quarter, :] = a2.total(h).astype(BF16)
    for h in range(2):
        start = rows // 2 + h * quarter
        dx_out[start : start + quarter, :] = b2.total(h).astype(BF16)
    links.drain()


def per_device(inputs, cotangent, gate_weight, up_weight, down_weight):
    rows, half = inputs.shape
    units, width = gate_weight.shape
    pad = -(-units // 16) * 16
    hidden = 2 * N * pad
    tokens = 2 * N * rows
    quarter = rows // 4
    vmem = pltpu.VMEM
    scratch = [
        vmem((N, 2, rows, width), BF16),
        vmem((N, 2, rows, width), BF16),
        vmem((3, hidden, width), BF16),
        vmem((hidden, tokens), F32),
        vmem((hidden, tokens), F32),
        vmem((hidden, tokens), BF16),
        vmem((hidden, 2 * rows), BF16),
        vmem((N, 2, rows, width), F32),
        vmem((2, rows // 2, width), F32),
        vmem((N, rows // 2, half), F32),
        vmem((hidden // 2, width), F32),
        vmem((hidden // 2, width), BF16),
        vmem((3, 2, rows // 2, width), BF16),
        vmem((3, 2, rows // 2, width), BF16),
        vmem((3, 2, quarter, half), BF16),
        vmem((3, 2, quarter, half), BF16),
        vmem((N, 3, 2, quarter, half), BF16),
        vmem((N, 3, 2, quarter, half), BF16),
        vmem((3, 2, quarter, half), BF16),
        vmem((3, 2, quarter, half), BF16),
        vmem((3, 2, pad, half), BF16),
        vmem((3, 2, pad, half), BF16),
        vmem((hidden // 2, width), BF16),
        pltpu.SemaphoreType.DMA((COPIES,)),
        pltpu.SemaphoreType.DMA((COPIES,)),
        pltpu.SemaphoreType.DMA((2,)),
    ]
    return pl.pallas_call(
        kernel,
        out_shape=(
            jax.ShapeDtypeStruct((rows, half), BF16),
            jax.ShapeDtypeStruct((units, width), BF16),
        ),
        in_specs=[pl.BlockSpec(memory_space=vmem)] * 5,
        out_specs=(pl.BlockSpec(memory_space=vmem),) * 2,
        scratch_shapes=scratch,
        compiler_params=pltpu.CompilerParams(
            collective_id=0, has_side_effects=True, vmem_limit_bytes=67043328
        ),
        name="swiglu_grads",
    )(inputs, cotangent, gate_weight, up_weight, down_weight)


def solution(mesh):
    torus = Mesh(
        mesh.devices.reshape(2, 4, 4, 2, mesh.shape["mp"]), ("dp_0", "dp_1", "dp_2", "dp_3", "mp")
    )
    return jax.shard_map(
        per_device,
        mesh=torus,
        in_specs=(P(DP, "mp"), P(DP, "mp"), P(MP_DP, None), P(MP_DP, None), P(MP_DP, None)),
        out_specs=(P(DP, "mp"), P(MP_DP, None)),
        check_vma=False,
    )
```

```python
import jax
import jax.numpy as jnp
from jax import lax
from jax.experimental import pallas as pl
from jax.experimental.pallas import tpu as pltpu
from jax.sharding import Mesh
from jax.sharding import PartitionSpec as P

DP = ("dp_0", "dp_1", "dp_2", "dp_3")
MP_DP = ("mp", "dp_0", "dp_1", "dp_2", "dp_3")
MESH = pl.DeviceIdType.MESH
F32 = jnp.float32
BF16 = jnp.bfloat16
N = 4
COPIES = 147
VMEM_LIMIT = 66400000
SLOT = (0, 1, 3, 2)


def dot(left, right, contract):
    return lax.dot_general(
        left, right, ((contract[:1], contract[1:]), ((), ())), preferred_element_type=F32
    )


class Links:
    def __init__(self, send, recv):
        self.send, self.recv, self.started = send, recv, []

    def copy(self, src, dst, device):
        k = len(self.started)
        c = pltpu.make_async_remote_copy(
            src_ref=src,
            dst_ref=dst,
            send_sem=self.send.at[k],
            recv_sem=self.recv.at[k],
            device_id=device,
            device_id_type=MESH,
        )
        c.start()
        self.started.append(c)
        return c

    def drain(self):
        for c in self.started:
            c.wait_send()


class Place:
    def __init__(self):
        self.x = lax.axis_index("dp_1")
        self.y = lax.axis_index("dp_2")
        self.c = lax.axis_index("dp_3")
        self.z = lax.axis_index("dp_0") * 2 + lax.axis_index("mp")

    def at_z(self, dz):
        z = lax.rem(self.z + (dz + N), N)
        return lax.div(z, 2), lax.rem(z, 2)

    def to(self, axis, step):
        if axis == "x":
            return {"dp_1": lax.rem(self.x + (step + N), N)}
        if axis == "y":
            return {"dp_2": lax.rem(self.y + (step + N), N)}
        if axis == "z":
            high, low = self.at_z(step)
            return {"dp_0": high, "mp": low}
        return {"dp_3": 1 - self.c}


class Tokens:
    def __init__(self, links, place, buf, half, p, q):
        self.links, self.place, self.buf, self.half = links, place, buf, half
        self.p, self.q = p, q
        self.rows = buf.shape[2]
        self.s2, self.f2 = {}, {}

    def slot(self, dx, dz, h):
        high, low = self.place.at_z(dz)
        rows = pl.ds(0, self.rows) if h is None else pl.ds(h * self.rows // 2, self.rows // 2)
        columns = pl.ds(pl.multiple_of(low * self.half, 128), self.half)
        return self.buf.at[SLOT[dx % N], high, rows, columns]

    def piece(self, kp, kq):
        return (kp, kq) if self.p == "x" else (kq, kp)

    def push(self, kp, kq, h, axis, step):
        dx, dz = self.piece(kp, kq)
        ex = step if axis == "x" else 0
        return self.links.copy(self.slot(dx, dz, h), self.slot(dx - ex, dz, h), self.place.to(axis, step))

    def start1(self):
        self.s1 = [self.push(0, 0, None, self.p, e) for e in (1, -1)]

    def both2(self, k, h):
        return [self.push(2 if k in ("lo", "hi") else k, 0, h, self.q, e) for e in (1, -1)]

    def start2(self):
        self.s2[0] = self.both2(0, None)

    def after1(self):
        for c in self.s1:
            c.wait_recv()

    def forward1(self):
        self.f1 = [self.push(-1, 0, 0, self.p, 1), self.push(1, 0, 1, self.p, -1)]

    def spread1(self):
        self.s2[-1] = self.both2(-1, None)
        self.s2[1] = self.both2(1, None)

    def after_f1(self):
        self.f1[0].wait_recv()
        self.s2["lo"] = self.both2("lo", 0)
        self.f1[1].wait_recv()
        self.s2["hi"] = self.both2("hi", 1)

    def after2(self, k):
        self.s2[k][0].wait_recv()
        a = self.push(k, -1, 0, self.q, 1)
        self.s2[k][1].wait_recv()
        b = self.push(k, 1, 1, self.q, -1)
        self.f2[k] = [a, b]

    def after2_opposite(self):
        self.s2["lo"][0].wait_recv()
        a = self.push(2, -1, 0, self.q, 1)
        self.s2["hi"][1].wait_recv()
        b = self.push(2, 1, 1, self.q, -1)
        self.s2["lo"][1].wait_recv()
        self.s2["hi"][0].wait_recv()
        self.f2[2] = [a, b]

    def after_f2(self, k):
        for c in self.f2[k]:
            c.wait_recv()


class Weight:
    def __init__(self, links, place, buf, pad):
        self.links, self.place, self.buf, self.pad = links, place, buf, pad
        self.width = buf.shape[1]
        self.core = []

    def slot(self, c, dy, h):
        rows = pl.ds((c * N + dy % N) * self.pad, self.pad)
        if h is None:
            return self.buf.at[rows, :]
        return self.buf.at[rows, pl.ds(h * self.width // 2, self.width // 2)]

    def cross(self, dy, h):
        self.core.append(
            self.links.copy(self.slot(0, dy, h), self.slot(1, dy, h), self.place.to("c", 1))
        )

    def turn(self, h, step):
        return self.links.copy(self.slot(0, 0, h), self.slot(0, -step, h), self.place.to("y", step))

    def start(self):
        self.s = [self.turn(0, 1), self.turn(1, -1), self.turn(1, 1), self.turn(0, -1)]
        self.cross(0, None)

    def after(self):
        self.s[0].wait_recv()
        a = self.links.copy(self.slot(0, -1, 0), self.slot(0, -2, 0), self.place.to("y", 1))
        self.s[1].wait_recv()
        b = self.links.copy(self.slot(0, 1, 1), self.slot(0, 2, 1), self.place.to("y", -1))
        self.f = [a, b]

    def after_rest(self):
        self.s[2].wait_recv()
        self.cross(-1, None)
        self.s[3].wait_recv()
        self.cross(1, None)

    def after_f(self):
        self.f[0].wait_recv()
        self.cross(2, 0)
        self.f[1].wait_recv()
        self.cross(2, 1)

    def finish(self):
        for c in self.core:
            c.wait_recv()


class Scatter:
    def __init__(self, links, place, axis, mine, send, recv):
        self.links, self.place, self.axis = links, place, axis
        self.mine, self.send, self.recv = mine, send, recv

    def go(self, value, u, h, step):
        self.send[u, h] = value.astype(BF16)
        return self.links.copy(
            self.send.at[u, h], self.recv.at[u, h], self.place.to(self.axis, step)
        )

    def first(self):
        self.a = self.go(self.mine(2, 0), 0, 0, 1)
        self.b = self.go(self.mine(2, 1), 0, 1, -1)

    def direct_right(self):
        self.r1 = self.go(self.mine(1, 1), 1, 1, 1)

    def direct_left(self):
        self.l0 = self.go(self.mine(-1, 0), 2, 0, -1)

    def second(self):
        self.a.wait_recv()
        self.r0 = self.go(self.mine(1, 0) + self.recv[0, 0].astype(F32), 1, 0, 1)
        self.b.wait_recv()
        self.l1 = self.go(self.mine(-1, 1) + self.recv[0, 1].astype(F32), 2, 1, -1)

    def total(self, h):
        (self.r1 if h else self.r0).wait_recv()
        (self.l1 if h else self.l0).wait_recv()
        return self.mine(0, h) + self.recv[1, h].astype(F32) + self.recv[2, h].astype(F32)


def kernel(
    x_ref, y_ref, g_ref, u_ref, d_ref, dx_out, dw_out,
    xb, yb, wb, win, gu, dgu, dgate, dx, ra, rb, dwf, dwr,
    a1s, a1r, a2s, a2r, b1s, b1r, b2s, b2r, ws, wr, wcs,
    send_sem, recv_sem, own_sem,
):
    place = Place()
    links = Links(send_sem, recv_sem)
    rows, half = x_ref.shape
    units, width = g_ref.shape
    hidden = wb.shape[1]
    pad = hidden // (2 * N)
    quarter = rows // 4
    block = 2 * rows

    barrier = pltpu.get_barrier_semaphore()
    peers = [("x", 1), ("x", -1), ("y", 1), ("y", -1), ("z", 1), ("z", -1), ("c", 1)]
    for axis, step in peers:
        pl.semaphore_signal(barrier, inc=1, device_id=place.to(axis, step), device_id_type=MESH)
    tx = Tokens(links, place, xb, half, "z", "x")
    ty = Tokens(links, place, yb, half, "x", "z")
    wg, wu, wd = (Weight(links, place, wb.at[m], pad) for m in range(3))
    pairs = [(x_ref, tx.slot(0, 0, None)), (y_ref, ty.slot(0, 0, None))]
    pairs += [(ref, win.at[m]) for m, ref in enumerate((g_ref, u_ref, d_ref))]
    loads = [pltpu.make_async_copy(a, b, own_sem.at[k]) for k, (a, b) in enumerate(pairs)]
    for c in loads:
        c.start()

    def place_weight(m):
        loads[2 + m].wait()
        if pad > units:
            low = units // 8 * 8
            wb[m, low:pad, :] = jnp.zeros((pad - low, width), BF16)
        wb[m, 0:units, :] = win[m]

    for c in loads[:2]:
        c.wait()
    pl.semaphore_wait(barrier, len(peers))
    tx.start1()
    ty.start1()
    tx.start2()
    ty.start2()
    place_weight(0)
    wg.start()
    place_weight(1)
    wu.start()
    place_weight(2)

    def spot(k):
        return SLOT[k % N]

    def forward(k, count):
        a = spot(k)
        tokens = xb[a : a + count].reshape(count * block, width)
        both = dot(tokens, wb[0:2].reshape(2 * hidden, width), (1, 1))
        gu[a : a + count] = both.reshape(count, block, 2 * hidden)

    def backward(k):
        a = spot(k)
        dh = dot(yb[a].reshape(block, width), wb[2], (1, 1))
        g = gu[a, :, 0:hidden]
        sig = jax.nn.sigmoid(g)
        dg = (dh * gu[a, :, hidden:] * sig * (1.0 + g * (1.0 - sig))).astype(BF16)
        dgu[:, 0:hidden] = dg
        dgu[:, hidden:] = (dh * (g * sig)).astype(BF16)
        part = dot(dgu[...], wb[0:2].reshape(2 * hidden, width), (1, 0))
        dx[a] = part.reshape(2, rows, width)
        dgate[:, a * block : (a + 1) * block] = dgu[:, 0:hidden].T

    def z_part(k, d, start):
        high, low = place.at_z(d)
        columns = pl.ds(pl.multiple_of(low * half, 128), half)
        return dx[spot(k), high, pl.ds(start, quarter), columns]

    def quarters(h):
        return slice(h * quarter, (h + 1) * quarter)

    a1 = [
        Scatter(
            links, place, "x", lambda d, h, j=j: z_part(d, j, h * quarter), a1s.at[j], a1r.at[j]
        )
        for j in range(N)
    ]
    a2 = Scatter(links, place, "z", lambda d, h: ra[d % N, quarters(h), :], a2s, a2r)
    b1 = [
        Scatter(
            links, place, "z",
            lambda d, h, k=k: z_part(k, d, rows // 2 + h * quarter),
            b1s.at[k], b1r.at[k],
        )
        for k in range(N)
    ]
    b2 = Scatter(links, place, "x", lambda d, h: rb[d % N, quarters(h), :], b2s, b2r)

    def dw_part(d, h):
        r = slice(d % N * pad, (d % N + 1) * pad)
        c = slice(h * half, (h + 1) * half)
        return dwf[r, c] + dwr[r, c].astype(F32)

    w1 = Scatter(links, place, "y", dw_part, ws, wr)
    order = (2, 1, 3, 0)

    def b1_start(k):
        b1[k % N].first()
        b1[k % N].direct_right()
        b1[k % N].direct_left()

    def end(stage, out, k):
        for h in range(2):
            out[k % N, quarters(h), :] = stage[k % N].total(h)

    tx.after1()
    ty.after1()
    tx.forward1()
    tx.spread1()
    ty.spread1()
    wg.after()
    wg.after_rest()
    wu.after()
    wd.start()
    tx.after_f1()
    ty.forward1()
    tx.after2(0)
    ty.after2(0)
    wu.after_rest()
    wg.after_f()
    tx.after2(-1)
    ty.after2(-1)
    wu.after_f()
    wg.finish()
    wu.finish()
    forward(0, 1)
    tx.after2(1)
    ty.after2(1)
    wd.after()
    tx.after2_opposite()
    wd.after_rest()
    forward(1, 1)
    ty.after_f1()
    wd.after_f()
    forward(-1, 1)
    wd.finish()
    ty.after_f2(-1)
    backward(-1)
    b1_start(-1)
    for j in order:
        a1[j].direct_left()
    ty.after2_opposite()
    ty.after_f2(1)
    backward(1)
    b1_start(1)
    for j in order:
        a1[j].direct_right()
    ty.after_f2(0)
    backward(0)
    b1_start(0)
    tx.after_f2(0)
    tx.after_f2(-1)
    tx.after_f2(1)
    tx.after_f2(2)
    forward(2, 1)
    b1[N - 1].second()
    b1[1].second()
    ty.after_f2(2)
    backward(2)
    for j in order:
        a1[j].first()
    b1_start(2)

    whole = xb[...].reshape(N * block, width)
    other = hidden // 2
    wcs[...] = dot(dgate[other:, :], whole, (1, 0)).astype(BF16)
    cross = links.copy(wcs, dwr, place.to("c", 1))
    b1[0].second()
    b1[2].second()
    a1[2].second()
    a1[1].second()
    dwf[...] = dot(dgate[0:other, :], whole, (1, 0))
    a1[3].second()
    a1[0].second()
    cross.wait_recv()
    w1.first()
    end(b1, rb, 2)
    b2.first()
    end(a1, ra, 2)
    a2.first()
    end(b1, rb, 3)
    b2.direct_left()
    end(b1, rb, 1)
    b2.direct_right()
    end(a1, ra, 1)
    a2.direct_right()
    end(a1, ra, 3)
    a2.direct_left()
    w1.direct_right()
    w1.direct_left()
    b2.second()
    a2.second()
    end(b1, rb, 0)
    end(a1, ra, 0)
    w1.second()
    for h in range(2):
        dx_out[quarters(2 + h), :] = b2.total(h).astype(BF16)
    for h in range(2):
        dx_out[quarters(h), :] = a2.total(h).astype(BF16)
    for h in range(2):
        dw_out[:, h * half : (h + 1) * half] = w1.total(h)[0:units].astype(BF16)
    links.drain()


def per_device(inputs, cotangent, gate_weight, up_weight, down_weight):
    rows, half = inputs.shape
    units, width = gate_weight.shape
    pad = -(-units // 16) * 16
    hidden = 2 * N * pad
    tokens = 2 * N * rows
    quarter = rows // 4
    vmem = pltpu.VMEM
    ring = (3, 2, quarter, half)
    scratch = [
        vmem((N, 2, rows, width), BF16),
        vmem((N, 2, rows, width), BF16),
        vmem((3, hidden, width), BF16),
        vmem((3, units, width), BF16),
        vmem((N, 2 * rows, 2 * hidden), F32),
        vmem((2 * rows, 2 * hidden), BF16),
        vmem((hidden, tokens), BF16),
        vmem((N, 2, rows, width), F32),
        vmem((N, rows // 2, half), F32),
        vmem((N, rows // 2, half), F32),
        vmem((hidden // 2, width), F32),
        vmem((hidden // 2, width), BF16),
        vmem((N,) + ring, BF16),
        vmem((N,) + ring, BF16),
        vmem(ring, BF16),
        vmem(ring, BF16),
        vmem((N,) + ring, BF16),
        vmem((N,) + ring, BF16),
        vmem(ring, BF16),
        vmem(ring, BF16),
        vmem((3, 2, pad, half), BF16),
        vmem((3, 2, pad, half), BF16),
        vmem((hidden // 2, width), BF16),
        pltpu.SemaphoreType.DMA((COPIES,)),
        pltpu.SemaphoreType.DMA((COPIES,)),
        pltpu.SemaphoreType.DMA((5,)),
    ]
    return pl.pallas_call(
        kernel,
        out_shape=(
            jax.ShapeDtypeStruct((rows, half), BF16),
            jax.ShapeDtypeStruct((units, width), BF16),
        ),
        in_specs=[pl.BlockSpec(memory_space=pltpu.HBM)] * 5,
        out_specs=(pl.BlockSpec(memory_space=vmem),) * 2,
        scratch_shapes=scratch,
        compiler_params=pltpu.CompilerParams(
            collective_id=0, has_side_effects=True, vmem_limit_bytes=VMEM_LIMIT
        ),
        name="swiglu_grads",
    )(inputs, cotangent, gate_weight, up_weight, down_weight)


def solution(mesh):
    torus = Mesh(
        mesh.devices.reshape(2, 4, 4, 2, mesh.shape["mp"]), ("dp_0", "dp_1", "dp_2", "dp_3", "mp")
    )
    return jax.shard_map(
        per_device,
        mesh=torus,
        in_specs=(P(DP, "mp"), P(DP, "mp"), P(MP_DP, None), P(MP_DP, None), P(MP_DP, None)),
        out_specs=(P(DP, "mp"), P(MP_DP, None)),
        check_vma=False,
    )
```

```python
import math

import jax
import jax.numpy as jnp
from jax import lax
from jax.experimental import pallas as pl
from jax.experimental.pallas import tpu as pltpu
from jax.sharding import Mesh
from jax.sharding import PartitionSpec as P

DP = ("dp_0", "dp_1", "dp_2", "dp_3")
MP_DP = ("mp", "dp_0", "dp_1", "dp_2", "dp_3")
MESH = pl.DeviceIdType.MESH
F32 = jnp.float32
BF16 = jnp.bfloat16
N = 4
GROUPS = 58
VMEM_LIMIT = 66400000
SLOT = (0, 1, 3, 2)


def dot(left, right, contract):
    return lax.dot_general(
        left, right, ((contract[:1], contract[1:]), ((), ())), preferred_element_type=F32
    )


class Group:
    def __init__(self, sem):
        self.sem = sem

    def wait(self, like):
        pltpu.make_async_copy(like, like, self.sem).wait()


class Links:
    def __init__(self, send, recv, limits):
        self.send, self.recv, self.limits = send, recv, limits
        self.groups = 0
        self.sent = [0] * len(limits)

    def group(self):
        self.groups += 1
        return Group(self.recv.at[self.groups - 1])

    def copy(self, src, dst, device, group, kinds=(0,)):
        size = math.prod(src.shape) * src.dtype.itemsize
        kind = next(k for k in kinds if self.sent[k] + size <= self.limits[k])
        self.sent[kind] += size
        pltpu.make_async_remote_copy(
            src_ref=src,
            dst_ref=dst,
            send_sem=self.send.at[kind],
            recv_sem=group.sem,
            device_id=device,
            device_id_type=MESH,
        ).start()

    def drain(self, refs):
        assert self.sent == self.limits, self.sent
        for k, ref in enumerate(refs):
            pltpu.make_async_copy(ref, ref, self.send.at[k]).wait()


class Place:
    def __init__(self):
        self.x = lax.axis_index("dp_1")
        self.y = lax.axis_index("dp_2")
        self.c = lax.axis_index("dp_3")
        self.z = lax.axis_index("dp_0") * 2 + lax.axis_index("mp")

    def at_z(self, dz):
        z = lax.rem(self.z + (dz + N), N)
        return lax.div(z, 2), lax.rem(z, 2)

    def to(self, axis, step):
        if axis == "x":
            return {"dp_1": lax.rem(self.x + (step + N), N)}
        if axis == "y":
            return {"dp_2": lax.rem(self.y + (step + N), N)}
        if axis == "z":
            high, low = self.at_z(step)
            return {"dp_0": high, "mp": low}
        return {"dp_3": 1 - self.c}


class Tokens:
    def __init__(self, links, place, buf, half, p, q):
        self.links, self.place, self.buf, self.half = links, place, buf, half
        self.p, self.q = p, q
        self.rows = buf.shape[2]
        self.s2, self.f2 = {}, {}

    def slot(self, dx, dz, h):
        high, low = self.place.at_z(dz)
        rows = pl.ds(0, self.rows) if h is None else pl.ds(h * self.rows // 2, self.rows // 2)
        columns = pl.ds(pl.multiple_of(low * self.half, 128), self.half)
        return self.buf.at[SLOT[dx % N], high, rows, columns]

    def piece(self, kp, kq):
        return (kp, kq) if self.p == "x" else (kq, kp)

    def push(self, kp, kq, h, axis, step, group):
        dx, dz = self.piece(kp, kq)
        ex = step if axis == "x" else 0
        self.links.copy(
            self.slot(dx, dz, h), self.slot(dx - ex, dz, h), self.place.to(axis, step), group
        )

    def pair(self, kp, kq, h, axis):
        group = self.links.group()
        for e in (1, -1):
            self.push(kp, kq, h, axis, e, group)
        return group

    def onward(self, pieces, axis):
        group = self.links.group()
        for (kp, kq), h, e in zip(pieces, (0, 1), (1, -1)):
            self.push(kp, kq, h, axis, e, group)
        return group

    def one(self):
        return self.buf.at[0, 0, :, 0 : self.half]

    def two(self):
        return self.buf.at[0, 0]

    def start1(self):
        self.s1 = self.pair(0, 0, None, self.p)

    def start2(self):
        self.s2[0] = self.pair(0, 0, None, self.q)

    def after1(self):
        self.s1.wait(self.two())

    def forward1(self):
        self.f1 = self.onward(((-1, 0), (1, 0)), self.p)

    def spread1(self):
        self.s2[-1] = self.pair(-1, 0, None, self.q)
        self.s2[1] = self.pair(1, 0, None, self.q)

    def after_f1(self):
        self.f1.wait(self.one())
        self.near = self.onward(((2, 0), (2, 0)), self.q)
        self.far = self.links.group()
        self.push(2, 0, 1, self.q, 1, self.far)
        self.push(2, 0, 0, self.q, -1, self.far)

    def after2(self, k):
        self.s2[k].wait(self.two())
        self.f2[k] = self.onward(((k, -1), (k, 1)), self.q)

    def after2_opposite(self):
        self.near.wait(self.one())
        self.f2[2] = self.onward(((2, -1), (2, 1)), self.q)

    def after2_rest(self):
        self.far.wait(self.one())

    def after_f2(self, k):
        self.f2[k].wait(self.one())


class Weight:
    def __init__(self, links, place, buf, pad):
        self.links, self.place, self.buf, self.pad = links, place, buf, pad
        self.width = buf.shape[1]

    def slot(self, c, dy, h):
        rows = pl.ds((c * N + dy % N) * self.pad, self.pad)
        if h is None:
            return self.buf.at[rows, :]
        return self.buf.at[rows, pl.ds(h * self.width // 2, self.width // 2)]

    def cross(self, dy):
        self.links.copy(
            self.slot(0, dy, None), self.slot(1, dy, None), self.place.to("c", 1), self.core, (1,)
        )

    def turn(self, dy, h, step, group):
        self.links.copy(
            self.slot(0, dy, h), self.slot(0, dy - step, h), self.place.to("y", step), group, (1,)
        )

    def one(self):
        return self.buf.at[0 : self.pad]

    def start(self):
        self.near, self.far, self.core = (self.links.group() for _ in range(3))
        self.turn(0, 0, 1, self.near)
        self.turn(0, 1, -1, self.near)
        self.turn(0, 1, 1, self.far)
        self.turn(0, 0, -1, self.far)
        self.cross(0)

    def after(self):
        self.near.wait(self.one())
        self.last = self.links.group()
        self.turn(-1, 0, 1, self.last)
        self.turn(1, 1, -1, self.last)

    def after_rest(self):
        self.far.wait(self.one())
        self.cross(-1)
        self.cross(1)

    def after_f(self):
        self.last.wait(self.one())
        self.cross(2)

    def finish(self):
        self.core.wait(self.buf.at[0 : N * self.pad])


class Scatter:
    def __init__(self, links, place, axis, mine, send, recv, like, kinds=(2,)):
        self.kinds = kinds
        self.links, self.place, self.axis = links, place, axis
        self.mine, self.send, self.recv, self.like = mine, send, recv, like
        self.early, self.late = links.group(), links.group()

    def go(self, value, u, h, step, group):
        self.send[u, h] = value.astype(BF16)
        self.links.copy(
            self.send.at[u, h], self.recv.at[u, h], self.place.to(self.axis, step), group,
            self.kinds,
        )

    def first(self):
        self.go(self.mine(2, 0), 0, 0, 1, self.early)
        self.go(self.mine(2, 1), 0, 1, -1, self.early)

    def direct_right(self):
        self.go(self.mine(1, 1), 1, 1, 1, self.late)

    def direct_left(self):
        self.go(self.mine(-1, 0), 2, 0, -1, self.late)

    def second(self):
        self.early.wait(self.like[0])
        self.go(self.mine(1, 0) + self.recv[0, 0].astype(F32), 1, 0, 1, self.late)
        self.go(self.mine(-1, 1) + self.recv[0, 1].astype(F32), 2, 1, -1, self.late)

    def totals(self):
        self.late.wait(self.like[1])
        return [
            self.mine(0, h) + self.recv[1, h].astype(F32) + self.recv[2, h].astype(F32)
            for h in range(2)
        ]


def kernel(
    x_ref, y_ref, g_ref, u_ref, d_ref, dx_out, dw_out,
    xb, yb, wb, win, gu, dgu, dgate, dx, ra, rb, dwf, dwr,
    a1s, a1r, a2s, a2r, b1s, b1r, b2s, b2r, ws, wr, wcs,
    send_sem, recv_sem, own_sem,
):
    place = Place()
    whole_bytes = math.prod(dx.shape) * 4
    links = Links(send_sem, recv_sem, [whole_bytes, whole_bytes, whole_bytes // 2])
    rows, half = x_ref.shape
    units, width = g_ref.shape
    hidden = wb.shape[1]
    pad = hidden // (2 * N)
    quarter = rows // 4
    block = 2 * rows

    barrier = pltpu.get_barrier_semaphore()
    peers = [("x", 1), ("x", -1), ("y", 1), ("y", -1), ("z", 1), ("z", -1), ("c", 1)]
    for axis, step in peers:
        pl.semaphore_signal(barrier, inc=1, device_id=place.to(axis, step), device_id_type=MESH)
    tx = Tokens(links, place, xb, half, "z", "x")
    ty = Tokens(links, place, yb, half, "x", "z")
    wg, wu, wd = (Weight(links, place, wb.at[m], pad) for m in range(3))
    pairs = [(x_ref, tx.slot(0, 0, None)), (y_ref, ty.slot(0, 0, None))]
    pairs += [(ref, win.at[m]) for m, ref in enumerate((g_ref, u_ref, d_ref))]
    loads = [pltpu.make_async_copy(a, b, own_sem.at[k]) for k, (a, b) in enumerate(pairs)]
    for c in loads:
        c.start()

    def place_weight(m):
        loads[2 + m].wait()
        if pad > units:
            low = units // 8 * 8
            wb[m, low:pad, :] = jnp.zeros((pad - low, width), BF16)
        wb[m, 0:units, :] = win[m]

    for c in loads[:2]:
        c.wait()
    pl.semaphore_wait(barrier, len(peers))
    tx.start1()
    ty.start1()
    tx.start2()
    ty.start2()
    place_weight(0)
    wg.start()
    place_weight(1)
    wu.start()
    place_weight(2)

    def spot(k):
        return SLOT[k % N]

    def forward(k, count):
        a = spot(k)
        tokens = xb[a : a + count].reshape(count * block, width)
        both = dot(tokens, wb[0:2].reshape(2 * hidden, width), (1, 1))
        gu[a : a + count] = both.reshape(count, block, 2 * hidden)

    def backward(k):
        a = spot(k)
        dh = dot(yb[a].reshape(block, width), wb[2], (1, 1))
        g = gu[a, :, 0:hidden]
        sig = jax.nn.sigmoid(g)
        dg = (dh * gu[a, :, hidden:] * sig * (1.0 + g * (1.0 - sig))).astype(BF16)
        dgu[:, 0:hidden] = dg
        dgu[:, hidden:] = (dh * (g * sig)).astype(BF16)
        part = dot(dgu[...], wb[0:2].reshape(2 * hidden, width), (1, 0))
        dx[a] = part.reshape(2, rows, width)
        dgate[:, a * block : (a + 1) * block] = dgu[:, 0:hidden].T

    def z_part(k, d, start):
        high, low = place.at_z(d)
        columns = pl.ds(pl.multiple_of(low * half, 128), half)
        return dx[spot(k), high, pl.ds(start, quarter), columns]

    def quarters(h):
        return slice(h * quarter, (h + 1) * quarter)

    like = (xb.at[0, 0, 0 : rows // 2, 0:half], xb.at[0, 0, :, 0:half])
    spare = (0, 1, 2)
    a1 = [
        Scatter(
            links, place, "x", lambda d, h, j=j: z_part(d, j, h * quarter),
            a1s.at[j], a1r.at[j], like,
        )
        for j in range(N)
    ]
    a2 = Scatter(links, place, "z", lambda d, h: ra[d % N, quarters(h), :], a2s, a2r, like, spare)
    b1 = [
        Scatter(
            links, place, "z",
            lambda d, h, k=k: z_part(k, d, rows // 2 + h * quarter),
            b1s.at[k], b1r.at[k], like,
        )
        for k in range(N)
    ]
    b2 = Scatter(links, place, "x", lambda d, h: rb[d % N, quarters(h), :], b2s, b2r, like, spare)

    def dw_part(d, h):
        r = slice(d % N * pad, (d % N + 1) * pad)
        c = slice(h * half, (h + 1) * half)
        return dwf[r, c] + dwr[r, c].astype(F32)

    like_w = (wb.at[0, 0:pad], wb.at[0, 0 : 2 * pad])
    w1 = Scatter(links, place, "y", dw_part, ws, wr, like_w)
    order = (2, 1, 3, 0)

    def b1_start(k):
        b1[k % N].first()
        b1[k % N].direct_right()
        b1[k % N].direct_left()

    def end(stage, out, k):
        for h, total in enumerate(stage[k % N].totals()):
            out[k % N, quarters(h), :] = total

    tx.after1()
    ty.after1()
    tx.forward1()
    tx.spread1()
    ty.spread1()
    wg.after()
    wg.after_rest()
    wu.after()
    wd.start()
    tx.after_f1()
    ty.forward1()
    tx.after2(0)
    ty.after2(0)
    wu.after_rest()
    wg.after_f()
    tx.after2(-1)
    ty.after2(-1)
    wu.after_f()
    wg.finish()
    wu.finish()
    forward(0, 1)
    tx.after2(1)
    ty.after2(1)
    wd.after()
    tx.after2_opposite()
    tx.after2_rest()
    wd.after_rest()
    forward(1, 1)
    ty.after_f1()
    wd.after_f()
    forward(-1, 1)
    wd.finish()
    ty.after_f2(-1)
    backward(-1)
    ty.after2_opposite()
    ty.after_f2(1)
    backward(1)
    for j in order:
        a1[j].direct_left()
        a1[j].direct_right()
    b1_start(-1)
    b1_start(1)
    ty.after_f2(0)
    backward(0)
    b1[0].first()
    tx.after_f2(0)
    tx.after_f2(-1)
    tx.after_f2(1)
    tx.after_f2(2)
    forward(2, 1)
    b1[N - 1].second()
    ty.after2_rest()
    ty.after_f2(2)
    backward(2)
    for j in order:
        a1[j].first()
    b1[2].first()
    b1[1].second()

    whole = xb[...].reshape(N * block, width)
    other = hidden // 2
    upper = slice(other // 2, other)
    lower = slice(0, other // 2)
    crossings = []
    for part in (upper, lower):
        wcs[part] = dot(dgate[other + part.start : other + part.stop], whole, (1, 0)).astype(BF16)
        crossings.append(links.group())
        links.copy(wcs.at[part], dwr.at[part], place.to("c", 1), crossings[-1], (1,))
    b1[2].direct_right()
    b1[2].direct_left()
    dwf[upper] = dot(dgate[upper], whole, (1, 0))
    b1[2].second()
    crossings[0].wait(dwr.at[upper])
    w1.first()
    dwf[lower] = dot(dgate[lower], whole, (1, 0))
    a1[2].second()
    a1[1].second()
    a1[3].second()
    a1[0].second()
    end(b1, rb, 2)
    b2.first()
    crossings[1].wait(dwr.at[lower])
    w1.direct_right()
    w1.direct_left()
    b1[0].second()
    b1[0].direct_right()
    b1[0].direct_left()
    end(b1, rb, 3)
    b2.direct_left()
    end(b1, rb, 1)
    b2.direct_right()
    w1.second()
    end(a1, ra, 2)
    a2.first()
    end(a1, ra, 1)
    a2.direct_right()
    end(a1, ra, 3)
    a2.direct_left()
    b2.second()
    end(b1, rb, 0)
    a2.second()
    end(a1, ra, 0)
    for h, total in enumerate(b2.totals()):
        dx_out[quarters(2 + h), :] = total.astype(BF16)
    for h, total in enumerate(a2.totals()):
        dx_out[quarters(h), :] = total.astype(BF16)
    for h, total in enumerate(w1.totals()):
        dw_out[:, h * half : (h + 1) * half] = total[0:units].astype(BF16)
    links.drain((dx, dx, xb))


def per_device(inputs, cotangent, gate_weight, up_weight, down_weight):
    rows, half = inputs.shape
    units, width = gate_weight.shape
    pad = -(-units // 16) * 16
    hidden = 2 * N * pad
    tokens = 2 * N * rows
    quarter = rows // 4
    vmem = pltpu.VMEM
    ring = (3, 2, quarter, half)
    scratch = [
        vmem((N, 2, rows, width), BF16),
        vmem((N, 2, rows, width), BF16),
        vmem((3, hidden, width), BF16),
        vmem((3, units, width), BF16),
        vmem((N, 2 * rows, 2 * hidden), F32),
        vmem((2 * rows, 2 * hidden), BF16),
        vmem((hidden, tokens), BF16),
        vmem((N, 2, rows, width), F32),
        vmem((N, rows // 2, half), F32),
        vmem((N, rows // 2, half), F32),
        vmem((hidden // 2, width), F32),
        vmem((hidden // 2, width), BF16),
        vmem((N,) + ring, BF16),
        vmem((N,) + ring, BF16),
        vmem(ring, BF16),
        vmem(ring, BF16),
        vmem((N,) + ring, BF16),
        vmem((N,) + ring, BF16),
        vmem(ring, BF16),
        vmem(ring, BF16),
        vmem((3, 2, pad, half), BF16),
        vmem((3, 2, pad, half), BF16),
        vmem((hidden // 2, width), BF16),
        pltpu.SemaphoreType.DMA((3,)),
        pltpu.SemaphoreType.DMA((GROUPS,)),
        pltpu.SemaphoreType.DMA((5,)),
    ]
    return pl.pallas_call(
        kernel,
        out_shape=(
            jax.ShapeDtypeStruct((rows, half), BF16),
            jax.ShapeDtypeStruct((units, width), BF16),
        ),
        in_specs=[pl.BlockSpec(memory_space=pltpu.HBM)] * 5,
        out_specs=(pl.BlockSpec(memory_space=vmem),) * 2,
        scratch_shapes=scratch,
        compiler_params=pltpu.CompilerParams(
            collective_id=0, has_side_effects=True, vmem_limit_bytes=VMEM_LIMIT
        ),
        name="swiglu_grads",
    )(inputs, cotangent, gate_weight, up_weight, down_weight)


def solution(mesh):
    torus = Mesh(
        mesh.devices.reshape(2, 4, 4, 2, mesh.shape["mp"]), ("dp_0", "dp_1", "dp_2", "dp_3", "mp")
    )
    return jax.shard_map(
        per_device,
        mesh=torus,
        in_specs=(P(DP, "mp"), P(DP, "mp"), P(MP_DP, None), P(MP_DP, None), P(MP_DP, None)),
        out_specs=(P(DP, "mp"), P(MP_DP, None)),
        check_vma=False,
    )
```

```python
import math

import jax
import jax.numpy as jnp
from jax import lax
from jax.experimental import pallas as pl
from jax.experimental.pallas import tpu as pltpu
from jax.sharding import Mesh
from jax.sharding import PartitionSpec as P

DP = ("dp_0", "dp_1", "dp_2", "dp_3")
MP_DP = ("mp", "dp_0", "dp_1", "dp_2", "dp_3")
MESH = pl.DeviceIdType.MESH
F32 = jnp.float32
BF16 = jnp.bfloat16
N = 4
GROUPS = 58
VMEM_LIMIT = 65000000
SLOT = (0, 1, 3, 2)


def dot(left, right, contract):
    return lax.dot_general(
        left, right, ((contract[:1], contract[1:]), ((), ())), preferred_element_type=F32
    )


class Group:
    def __init__(self, sem):
        self.sem = sem

    def wait(self, like):
        pltpu.make_async_copy(like, like, self.sem).wait()


class Links:
    def __init__(self, send, recv, limits):
        self.send, self.recv, self.limits = send, recv, limits
        self.groups = 0
        self.sent = [0] * len(limits)

    def group(self):
        self.groups += 1
        return Group(self.recv.at[self.groups - 1])

    def copy(self, src, dst, device, group, kinds=(0,)):
        size = math.prod(src.shape) * src.dtype.itemsize
        kind = next(k for k in kinds if self.sent[k] + size <= self.limits[k])
        self.sent[kind] += size
        pltpu.make_async_remote_copy(
            src_ref=src,
            dst_ref=dst,
            send_sem=self.send.at[kind],
            recv_sem=group.sem,
            device_id=device,
            device_id_type=MESH,
        ).start()

    def drain(self, refs):
        assert self.sent == self.limits, self.sent
        for k, ref in enumerate(refs):
            pltpu.make_async_copy(ref, ref, self.send.at[k]).wait()


class Place:
    def __init__(self):
        self.x = lax.axis_index("dp_1")
        self.y = lax.axis_index("dp_2")
        self.c = lax.axis_index("dp_3")
        self.z = lax.axis_index("dp_0") * 2 + lax.axis_index("mp")

    def at_z(self, dz):
        z = lax.rem(self.z + (dz + N), N)
        return lax.div(z, 2), lax.rem(z, 2)

    def to(self, axis, step):
        if axis == "x":
            return {"dp_1": lax.rem(self.x + (step + N), N)}
        if axis == "y":
            return {"dp_2": lax.rem(self.y + (step + N), N)}
        if axis == "z":
            high, low = self.at_z(step)
            return {"dp_0": high, "mp": low}
        return {"dp_3": 1 - self.c}


class Tokens:
    def __init__(self, links, place, buf, half, p, q):
        self.links, self.place, self.buf, self.half = links, place, buf, half
        self.p, self.q = p, q
        self.rows = buf.shape[2]
        self.s2, self.f2 = {}, {}

    def slot(self, dx, dz, h):
        high, low = self.place.at_z(dz)
        rows = pl.ds(0, self.rows) if h is None else pl.ds(h * self.rows // 2, self.rows // 2)
        columns = pl.ds(pl.multiple_of(low * self.half, 128), self.half)
        return self.buf.at[SLOT[dx % N], high, rows, columns]

    def piece(self, kp, kq):
        return (kp, kq) if self.p == "x" else (kq, kp)

    def push(self, kp, kq, h, axis, step, group):
        dx, dz = self.piece(kp, kq)
        ex = step if axis == "x" else 0
        self.links.copy(
            self.slot(dx, dz, h), self.slot(dx - ex, dz, h), self.place.to(axis, step), group
        )

    def pair(self, kp, kq, h, axis):
        group = self.links.group()
        for e in (1, -1):
            self.push(kp, kq, h, axis, e, group)
        return group

    def onward(self, pieces, axis):
        group = self.links.group()
        for (kp, kq), h, e in zip(pieces, (0, 1), (1, -1)):
            self.push(kp, kq, h, axis, e, group)
        return group

    def one(self):
        return self.buf.at[0, 0, :, 0 : self.half]

    def two(self):
        return self.buf.at[0, 0]

    def start1(self):
        self.s1 = self.pair(0, 0, None, self.p)

    def start2(self):
        self.s2[0] = self.pair(0, 0, None, self.q)

    def after1(self):
        self.s1.wait(self.two())

    def forward1(self):
        self.f1 = self.onward(((-1, 0), (1, 0)), self.p)

    def spread1(self):
        self.s2[-1] = self.pair(-1, 0, None, self.q)
        self.s2[1] = self.pair(1, 0, None, self.q)

    def after_f1(self):
        self.f1.wait(self.one())
        self.near = self.onward(((2, 0), (2, 0)), self.q)
        self.far = self.links.group()
        self.push(2, 0, 1, self.q, 1, self.far)
        self.push(2, 0, 0, self.q, -1, self.far)

    def after2(self, k):
        self.s2[k].wait(self.two())
        self.f2[k] = self.onward(((k, -1), (k, 1)), self.q)

    def after2_opposite(self):
        self.near.wait(self.one())
        self.f2[2] = self.onward(((2, -1), (2, 1)), self.q)

    def after2_rest(self):
        self.far.wait(self.one())

    def after_f2(self, k):
        self.f2[k].wait(self.one())


class Weight:
    def __init__(self, links, place, buf, pad):
        self.links, self.place, self.buf, self.pad = links, place, buf, pad
        self.width = buf.shape[1]

    def slot(self, c, dy, h):
        rows = pl.ds((c * N + dy % N) * self.pad, self.pad)
        if h is None:
            return self.buf.at[rows, :]
        return self.buf.at[rows, pl.ds(h * self.width // 2, self.width // 2)]

    def cross(self, dy):
        self.links.copy(
            self.slot(0, dy, None), self.slot(1, dy, None), self.place.to("c", 1), self.core, (1,)
        )

    def turn(self, dy, h, step, group):
        self.links.copy(
            self.slot(0, dy, h), self.slot(0, dy - step, h), self.place.to("y", step), group, (1,)
        )

    def one(self):
        return self.buf.at[0 : self.pad]

    def start(self):
        self.near, self.far, self.core = (self.links.group() for _ in range(3))
        self.turn(0, 0, 1, self.near)
        self.turn(0, 1, -1, self.near)
        self.turn(0, 1, 1, self.far)
        self.turn(0, 0, -1, self.far)
        self.cross(0)

    def after(self):
        self.near.wait(self.one())
        self.last = self.links.group()
        self.turn(-1, 0, 1, self.last)
        self.turn(1, 1, -1, self.last)

    def after_rest(self):
        self.far.wait(self.one())
        self.cross(-1)
        self.cross(1)

    def after_f(self):
        self.last.wait(self.one())
        self.cross(2)

    def finish(self):
        self.core.wait(self.buf.at[0 : N * self.pad])


class Scatter:
    def __init__(self, links, place, axis, mine, send, recv, like, kinds=(2,)):
        self.kinds = kinds
        self.links, self.place, self.axis = links, place, axis
        self.mine, self.send, self.recv, self.like = mine, send, recv, like
        self.early, self.late = links.group(), links.group()

    def go(self, value, u, h, step, group):
        self.send[u, h] = value.astype(BF16)
        self.links.copy(
            self.send.at[u, h], self.recv.at[u, h], self.place.to(self.axis, step), group,
            self.kinds,
        )

    def first(self):
        self.go(self.mine(2, 0), 0, 0, 1, self.early)
        self.go(self.mine(2, 1), 0, 1, -1, self.early)

    def direct_right(self):
        self.go(self.mine(1, 1), 1, 1, 1, self.late)

    def direct_left(self):
        self.go(self.mine(-1, 0), 2, 0, -1, self.late)

    def second(self):
        self.early.wait(self.like[0])
        self.go(self.mine(1, 0) + self.recv[0, 0].astype(F32), 1, 0, 1, self.late)
        self.go(self.mine(-1, 1) + self.recv[0, 1].astype(F32), 2, 1, -1, self.late)

    def totals(self):
        self.late.wait(self.like[1])
        return [
            self.mine(0, h) + self.recv[1, h].astype(F32) + self.recv[2, h].astype(F32)
            for h in range(2)
        ]


def kernel(
    x_ref, y_ref, g_ref, u_ref, d_ref, dx_out, dw_out,
    xb, yb, wb, win, gu, dgu, dgate, dx, ra, rb, dwf, dwr,
    a1s, a1r, a2s, a2r, b1s, b1r, b2s, b2r, ws, wr, wcs,
    send_sem, recv_sem, own_sem,
):
    place = Place()
    whole_bytes = math.prod(dx.shape) * 4
    links = Links(send_sem, recv_sem, [whole_bytes, whole_bytes, whole_bytes // 2])
    rows, half = x_ref.shape
    units, width = g_ref.shape
    hidden = wb.shape[1]
    pad = hidden // (2 * N)
    quarter = rows // 4
    block = 2 * rows

    barrier = pltpu.get_barrier_semaphore()
    peers = [("x", 1), ("x", -1), ("y", 1), ("y", -1), ("z", 1), ("z", -1), ("c", 1)]
    for axis, step in peers:
        pl.semaphore_signal(barrier, inc=1, device_id=place.to(axis, step), device_id_type=MESH)
    tx = Tokens(links, place, xb, half, "z", "x")
    ty = Tokens(links, place, yb, half, "x", "z")
    wg, wu, wd = (Weight(links, place, wb.at[m], pad) for m in range(3))
    pairs = [(x_ref, tx.slot(0, 0, None)), (y_ref, ty.slot(0, 0, None))]
    pairs += [(ref, win.at[m]) for m, ref in enumerate((g_ref, u_ref, d_ref))]
    loads = [pltpu.make_async_copy(a, b, own_sem.at[k]) for k, (a, b) in enumerate(pairs)]
    for c in loads:
        c.start()

    def place_weight(m):
        loads[2 + m].wait()
        if pad > units:
            low = units // 8 * 8
            wb[m, low:pad, :] = jnp.zeros((pad - low, width), BF16)
        wb[m, 0:units, :] = win[m]

    for c in loads[:2]:
        c.wait()
    pl.semaphore_wait(barrier, len(peers))
    tx.start1()
    ty.start1()
    tx.start2()
    ty.start2()
    place_weight(0)
    wg.start()
    place_weight(1)
    wu.start()
    place_weight(2)

    def spot(k):
        return SLOT[k % N]

    def forward(k, count):
        a = spot(k)
        pl.delay(1)
        tokens = xb[a : a + count].reshape(count * block, width)
        both = dot(tokens, wb[0:2].reshape(2 * hidden, width), (1, 1))
        gu[a : a + count] = both.reshape(count, block, 2 * hidden)
        pl.delay(1)

    def backward(k):
        a = spot(k)
        pl.delay(1)
        dh = dot(yb[a].reshape(block, width), wb[2], (1, 1))
        g = gu[a, :, 0:hidden]
        sig = jax.nn.sigmoid(g)
        dg = (dh * gu[a, :, hidden:] * sig * (1.0 + g * (1.0 - sig))).astype(BF16)
        dgu[:, 0:hidden] = dg
        dgu[:, hidden:] = (dh * (g * sig)).astype(BF16)
        part = dot(dgu[...], wb[0:2].reshape(2 * hidden, width), (1, 0))
        dx[a] = part.reshape(2, rows, width)
        dgate[:, a * block : (a + 1) * block] = dgu[:, 0:hidden].T
        pl.delay(1)

    def z_part(k, d, start):
        high, low = place.at_z(d)
        columns = pl.ds(pl.multiple_of(low * half, 128), half)
        return dx[spot(k), high, pl.ds(start, quarter), columns]

    def quarters(h):
        return slice(h * quarter, (h + 1) * quarter)

    like = (xb.at[0, 0, 0 : rows // 2, 0:half], xb.at[0, 0, :, 0:half])
    spare = (0, 1, 2)
    a1 = [
        Scatter(
            links, place, "x", lambda d, h, j=j: z_part(d, j, h * quarter),
            a1s.at[j], a1r.at[j], like,
        )
        for j in range(N)
    ]
    a2 = Scatter(links, place, "z", lambda d, h: ra[d % N, quarters(h), :], a2s, a2r, like, spare)
    b1 = [
        Scatter(
            links, place, "z",
            lambda d, h, k=k: z_part(k, d, rows // 2 + h * quarter),
            b1s.at[k], b1r.at[k], like,
        )
        for k in range(N)
    ]
    b2 = Scatter(links, place, "x", lambda d, h: rb[d % N, quarters(h), :], b2s, b2r, like, spare)

    def dw_part(d, h):
        r = slice(d % N * pad, (d % N + 1) * pad)
        c = slice(h * half, (h + 1) * half)
        return dwf[r, c] + dwr[r, c].astype(F32)

    like_w = (wb.at[0, 0:pad], wb.at[0, 0 : 2 * pad])
    w1 = Scatter(links, place, "y", dw_part, ws, wr, like_w)
    order = (2, 1, 3, 0)

    def end(stage, out, k):
        for h, total in enumerate(stage[k % N].totals()):
            out[k % N, quarters(h), :] = total

    tx.after1()
    ty.after1()
    tx.forward1()
    tx.spread1()
    ty.spread1()
    wg.after()
    wg.after_rest()
    wu.after()
    wd.start()
    tx.after_f1()
    ty.forward1()
    tx.after2(0)
    ty.after2(0)
    wu.after_rest()
    wg.after_f()
    tx.after2(-1)
    ty.after2(-1)
    wu.after_f()
    wg.finish()
    wu.finish()
    forward(0, 1)
    tx.after2(1)
    ty.after2(1)
    wd.after()
    tx.after2_opposite()
    tx.after2_rest()
    wd.after_rest()
    forward(1, 1)
    ty.after_f1()
    wd.after_f()
    forward(-1, 1)
    wd.finish()
    ty.after_f2(-1)
    backward(-1)
    ty.after2_opposite()
    ty.after_f2(1)
    backward(1)
    for j in order:
        a1[j].direct_left()
        a1[j].direct_right()
    for k in (3, 1):
        b1[k].first()
    for k in (3, 1):
        b1[k].direct_right()
        b1[k].direct_left()
    ty.after_f2(0)
    tx.after_f2(0)
    tx.after_f2(-1)
    tx.after_f2(1)
    tx.after_f2(2)
    forward(2, 1)
    ty.after2_rest()
    ty.after_f2(2)
    backward(2)
    for j in order:
        a1[j].first()
    b1[2].first()
    b1[2].direct_right()
    b1[2].direct_left()
    backward(0)
    b1[3].second()
    b1[1].second()

    whole = xb[...].reshape(N * block, width)
    other = hidden // 2
    upper = slice(other // 2, other)
    lower = slice(0, other // 2)
    crossings = []

    def other_rows(part):
        pl.delay(1)
        wcs[part] = dot(dgate[other + part.start : other + part.stop], whole, (1, 0)).astype(BF16)
        crossings.append(links.group())
        links.copy(wcs.at[part], dwr.at[part], place.to("c", 1), crossings[-1], (1,))
        pl.delay(1)

    def own_rows(part):
        pl.delay(1)
        dwf[part] = dot(dgate[part], whole, (1, 0))
        pl.delay(1)

    other_rows(upper)
    b1[2].second()
    a1[2].second()
    other_rows(lower)
    a1[1].second()
    a1[3].second()
    own_rows(upper)
    crossings[0].wait(dwr.at[upper])
    w1.first()
    a1[0].second()
    b1[0].first()
    own_rows(lower)
    end(b1, rb, 2)
    b2.first()
    crossings[1].wait(dwr.at[lower])
    w1.direct_right()
    w1.direct_left()
    end(a1, ra, 2)
    a2.first()
    end(b1, rb, 3)
    b2.direct_left()
    end(b1, rb, 1)
    b2.direct_right()
    end(a1, ra, 1)
    a2.direct_right()
    end(a1, ra, 3)
    a2.direct_left()
    b1[0].second()
    b1[0].direct_right()
    b1[0].direct_left()
    w1.second()
    b2.second()
    a2.second()
    end(a1, ra, 0)
    end(b1, rb, 0)
    for h, total in enumerate(b2.totals()):
        dx_out[quarters(2 + h), :] = total.astype(BF16)
    for h, total in enumerate(a2.totals()):
        dx_out[quarters(h), :] = total.astype(BF16)
    for h, total in enumerate(w1.totals()):
        dw_out[:, h * half : (h + 1) * half] = total[0:units].astype(BF16)
    links.drain((dx, dx, xb))


def per_device(inputs, cotangent, gate_weight, up_weight, down_weight):
    rows, half = inputs.shape
    units, width = gate_weight.shape
    pad = -(-units // 16) * 16
    hidden = 2 * N * pad
    tokens = 2 * N * rows
    quarter = rows // 4
    vmem = pltpu.VMEM
    ring = (3, 2, quarter, half)
    scratch = [
        vmem((N, 2, rows, width), BF16),
        vmem((N, 2, rows, width), BF16),
        vmem((3, hidden, width), BF16),
        vmem((3, units, width), BF16),
        vmem((N, 2 * rows, 2 * hidden), F32),
        vmem((2 * rows, 2 * hidden), BF16),
        vmem((hidden, tokens), BF16),
        vmem((N, 2, rows, width), F32),
        vmem((N, rows // 2, half), F32),
        vmem((N, rows // 2, half), F32),
        vmem((hidden // 2, width), F32),
        vmem((hidden // 2, width), BF16),
        vmem((N,) + ring, BF16),
        vmem((N,) + ring, BF16),
        vmem(ring, BF16),
        vmem(ring, BF16),
        vmem((N,) + ring, BF16),
        vmem((N,) + ring, BF16),
        vmem(ring, BF16),
        vmem(ring, BF16),
        vmem((3, 2, pad, half), BF16),
        vmem((3, 2, pad, half), BF16),
        vmem((hidden // 2, width), BF16),
        pltpu.SemaphoreType.DMA((3,)),
        pltpu.SemaphoreType.DMA((GROUPS,)),
        pltpu.SemaphoreType.DMA((5,)),
    ]
    return pl.pallas_call(
        kernel,
        out_shape=(
            vmem((rows, half), BF16),
            vmem((units, width), BF16),
        ),
        in_specs=[pl.BlockSpec(memory_space=pltpu.HBM)] * 5,
        out_specs=(pl.BlockSpec(memory_space=vmem),) * 2,
        scratch_shapes=scratch,
        compiler_params=pltpu.CompilerParams(
            collective_id=0, has_side_effects=True, vmem_limit_bytes=VMEM_LIMIT
        ),
        name="swiglu_grads",
    )(inputs, cotangent, gate_weight, up_weight, down_weight)


def solution(mesh):
    torus = Mesh(
        mesh.devices.reshape(2, 4, 4, 2, mesh.shape["mp"]), ("dp_0", "dp_1", "dp_2", "dp_3", "mp")
    )
    return jax.shard_map(
        per_device,
        mesh=torus,
        in_specs=(P(DP, "mp"), P(DP, "mp"), P(MP_DP, None), P(MP_DP, None), P(MP_DP, None)),
        out_specs=(P(DP, "mp"), P(MP_DP, None)),
        check_vma=False,
    )
```

```python
import math

import jax
import jax.numpy as jnp
from jax import lax
from jax.experimental import pallas as pl
from jax.experimental.pallas import tpu as pltpu
from jax.sharding import Mesh
from jax.sharding import PartitionSpec as P

DP = ("dp_0", "dp_1", "dp_2", "dp_3")
MP_DP = ("mp", "dp_0", "dp_1", "dp_2", "dp_3")
MESH = pl.DeviceIdType.MESH
F32 = jnp.float32
BF16 = jnp.bfloat16
N = 4
GROUPS = 58
VMEM_LIMIT = 65000000
SLOT = (0, 1, 3, 2)


def dot(left, right, contract):
    return lax.dot_general(
        left, right, ((contract[:1], contract[1:]), ((), ())), preferred_element_type=F32
    )


class Group:
    def __init__(self, sem):
        self.sem = sem

    def wait(self, like):
        pltpu.make_async_copy(like, like, self.sem).wait()


class Links:
    def __init__(self, send, recv, limits):
        self.send, self.recv, self.limits = send, recv, limits
        self.groups = 0
        self.sent = [0] * len(limits)

    def group(self):
        self.groups += 1
        return Group(self.recv.at[self.groups - 1])

    def copy(self, src, dst, device, group, kinds=(0,)):
        size = math.prod(src.shape) * src.dtype.itemsize
        kind = next(k for k in kinds if self.sent[k] + size <= self.limits[k])
        self.sent[kind] += size
        pltpu.make_async_remote_copy(
            src_ref=src,
            dst_ref=dst,
            send_sem=self.send.at[kind],
            recv_sem=group.sem,
            device_id=device,
            device_id_type=MESH,
        ).start()

    def drain(self, refs):
        assert self.sent == self.limits, self.sent
        for k, ref in enumerate(refs):
            pltpu.make_async_copy(ref, ref, self.send.at[k]).wait()


class Place:
    def __init__(self):
        self.x = lax.axis_index("dp_1")
        self.y = lax.axis_index("dp_2")
        self.c = lax.axis_index("dp_3")
        self.z = lax.axis_index("dp_0") * 2 + lax.axis_index("mp")

    def at_z(self, dz):
        z = lax.rem(self.z + (dz + N), N)
        return lax.div(z, 2), lax.rem(z, 2)

    def to(self, axis, step):
        if axis == "x":
            return {"dp_1": lax.rem(self.x + (step + N), N)}
        if axis == "y":
            return {"dp_2": lax.rem(self.y + (step + N), N)}
        if axis == "z":
            high, low = self.at_z(step)
            return {"dp_0": high, "mp": low}
        return {"dp_3": 1 - self.c}


class Tokens:
    def __init__(self, links, place, buf, half, p, q):
        self.links, self.place, self.buf, self.half = links, place, buf, half
        self.p, self.q = p, q
        self.rows = buf.shape[2]
        self.s2, self.f2 = {}, {}

    def slot(self, dx, dz, h):
        high, low = self.place.at_z(dz)
        rows = pl.ds(0, self.rows) if h is None else pl.ds(h * self.rows // 2, self.rows // 2)
        columns = pl.ds(pl.multiple_of(low * self.half, 128), self.half)
        return self.buf.at[SLOT[dx % N], high, rows, columns]

    def piece(self, kp, kq):
        return (kp, kq) if self.p == "x" else (kq, kp)

    def push(self, kp, kq, h, axis, step, group):
        dx, dz = self.piece(kp, kq)
        ex = step if axis == "x" else 0
        self.links.copy(
            self.slot(dx, dz, h), self.slot(dx - ex, dz, h), self.place.to(axis, step), group
        )

    def pair(self, kp, kq, h, axis):
        group = self.links.group()
        for e in (1, -1):
            self.push(kp, kq, h, axis, e, group)
        return group

    def onward(self, pieces, axis):
        group = self.links.group()
        for (kp, kq), h, e in zip(pieces, (0, 1), (1, -1)):
            self.push(kp, kq, h, axis, e, group)
        return group

    def one(self):
        return self.buf.at[0, 0, :, 0 : self.half]

    def two(self):
        return self.buf.at[0, 0]

    def start1(self):
        self.s1 = self.pair(0, 0, None, self.p)

    def start2(self):
        self.s2[0] = self.pair(0, 0, None, self.q)

    def after1(self):
        self.s1.wait(self.two())

    def forward1(self):
        self.f1 = self.onward(((-1, 0), (1, 0)), self.p)

    def spread1(self):
        self.s2[-1] = self.pair(-1, 0, None, self.q)
        self.s2[1] = self.pair(1, 0, None, self.q)

    def after_f1(self):
        self.f1.wait(self.one())
        self.near = self.onward(((2, 0), (2, 0)), self.q)
        self.far = self.links.group()
        self.push(2, 0, 1, self.q, 1, self.far)
        self.push(2, 0, 0, self.q, -1, self.far)

    def after2(self, k):
        self.s2[k].wait(self.two())
        self.f2[k] = self.onward(((k, -1), (k, 1)), self.q)

    def after2_opposite(self):
        self.near.wait(self.one())
        self.f2[2] = self.onward(((2, -1), (2, 1)), self.q)

    def after2_rest(self):
        self.far.wait(self.one())

    def after_f2(self, k):
        self.f2[k].wait(self.one())


class Weight:
    def __init__(self, links, place, buf, pad):
        self.links, self.place, self.buf, self.pad = links, place, buf, pad
        self.width = buf.shape[1]

    def slot(self, c, dy, h):
        rows = pl.ds((c * N + dy % N) * self.pad, self.pad)
        if h is None:
            return self.buf.at[rows, :]
        return self.buf.at[rows, pl.ds(h * self.width // 2, self.width // 2)]

    def cross(self, dy):
        self.links.copy(
            self.slot(0, dy, None), self.slot(1, dy, None), self.place.to("c", 1), self.core, (1,)
        )

    def turn(self, dy, h, step, group):
        self.links.copy(
            self.slot(0, dy, h), self.slot(0, dy - step, h), self.place.to("y", step), group, (1,)
        )

    def one(self):
        return self.buf.at[0 : self.pad]

    def start(self):
        self.near, self.far, self.core = (self.links.group() for _ in range(3))
        self.turn(0, 0, 1, self.near)
        self.turn(0, 1, -1, self.near)
        self.turn(0, 1, 1, self.far)
        self.turn(0, 0, -1, self.far)
        self.cross(0)

    def after(self):
        self.near.wait(self.one())
        self.last = self.links.group()
        self.turn(-1, 0, 1, self.last)
        self.turn(1, 1, -1, self.last)

    def after_rest(self):
        self.far.wait(self.one())
        self.cross(-1)
        self.cross(1)

    def after_f(self):
        self.last.wait(self.one())
        self.cross(2)

    def finish(self):
        self.core.wait(self.buf.at[0 : N * self.pad])


class Scatter:
    def __init__(self, links, place, axis, mine, send, recv, like, kinds=(2,)):
        self.kinds = kinds
        self.links, self.place, self.axis = links, place, axis
        self.mine, self.send, self.recv, self.like = mine, send, recv, like
        self.early, self.late = links.group(), links.group()

    def go(self, value, u, h, step, group):
        self.send[u, h] = value.astype(BF16)
        self.links.copy(
            self.send.at[u, h], self.recv.at[u, h], self.place.to(self.axis, step), group,
            self.kinds,
        )

    def first(self):
        self.go(self.mine(2, 0), 0, 0, 1, self.early)
        self.go(self.mine(2, 1), 0, 1, -1, self.early)

    def direct_right(self):
        self.go(self.mine(1, 1), 1, 1, 1, self.late)

    def direct_left(self):
        self.go(self.mine(-1, 0), 2, 0, -1, self.late)

    def second(self):
        self.early.wait(self.like[0])
        self.go(self.mine(1, 0) + self.recv[0, 0].astype(F32), 1, 0, 1, self.late)
        self.go(self.mine(-1, 1) + self.recv[0, 1].astype(F32), 2, 1, -1, self.late)

    def totals(self):
        self.late.wait(self.like[1])
        return [
            self.mine(0, h) + self.recv[1, h].astype(F32) + self.recv[2, h].astype(F32)
            for h in range(2)
        ]


def kernel(
    x_ref, y_ref, g_ref, u_ref, d_ref, dx_out, dw_out,
    xb, yb, wb, win, gu, dgu, dgate, dx, ra, rb, dwf, dwr,
    a1s, a1r, a2s, a2r, b1s, b1r, b2s, b2r, ws, wr, wcs,
    send_sem, recv_sem, own_sem,
):
    place = Place()
    whole_bytes = math.prod(dx.shape) * 4
    links = Links(send_sem, recv_sem, [whole_bytes, whole_bytes, whole_bytes // 2])
    rows, half = x_ref.shape
    units, width = g_ref.shape
    hidden = wb.shape[1]
    pad = hidden // (2 * N)
    quarter = rows // 4
    block = 2 * rows

    barrier = pltpu.get_barrier_semaphore()
    peers = [("x", 1), ("x", -1), ("y", 1), ("y", -1), ("z", 1), ("z", -1), ("c", 1)]
    for axis, step in peers:
        pl.semaphore_signal(barrier, inc=1, device_id=place.to(axis, step), device_id_type=MESH)
    tx = Tokens(links, place, xb, half, "z", "x")
    ty = Tokens(links, place, yb, half, "x", "z")
    wg, wu, wd = (Weight(links, place, wb.at[m], pad) for m in range(3))
    pairs = [(x_ref, tx.slot(0, 0, None)), (y_ref, ty.slot(0, 0, None))]
    pairs += [(ref, win.at[m]) for m, ref in enumerate((g_ref, u_ref, d_ref))]
    loads = [pltpu.make_async_copy(a, b, own_sem.at[k]) for k, (a, b) in enumerate(pairs)]
    for c in loads:
        c.start()

    def place_weight(m):
        loads[2 + m].wait()
        if pad > units:
            low = units // 8 * 8
            wb[m, low:pad, :] = jnp.zeros((pad - low, width), BF16)
        wb[m, 0:units, :] = win[m]

    for c in loads[:2]:
        c.wait()
    pl.semaphore_wait(barrier, len(peers))
    tx.start1()
    ty.start1()
    tx.start2()
    ty.start2()
    place_weight(0)
    wg.start()
    place_weight(1)
    wu.start()
    place_weight(2)

    def spot(k):
        return SLOT[k % N]

    def forward(k, count):
        a = spot(k)
        pl.delay(1)
        tokens = xb[a : a + count].reshape(count * block, width)
        both = dot(tokens, wb[0:2].reshape(2 * hidden, width), (1, 1))
        gu[a : a + count] = both.reshape(count, block, 2 * hidden)
        pl.delay(1)

    def backward(k):
        a = spot(k)
        pl.delay(1)
        dh = dot(yb[a].reshape(block, width), wb[2], (1, 1))
        g = gu[a, :, 0:hidden]
        sig = jax.nn.sigmoid(g)
        dg = (dh * gu[a, :, hidden:] * sig * (1.0 + g * (1.0 - sig))).astype(BF16)
        dgu[:, 0:hidden] = dg
        dgu[:, hidden:] = (dh * (g * sig)).astype(BF16)
        part = dot(dgu[...], wb[0:2].reshape(2 * hidden, width), (1, 0))
        dx[a] = part.reshape(2, rows, width)
        dgate[:, a * block : (a + 1) * block] = dgu[:, 0:hidden].T
        pl.delay(1)

    def z_part(k, d, start):
        high, low = place.at_z(d)
        columns = pl.ds(pl.multiple_of(low * half, 128), half)
        return dx[spot(k), high, pl.ds(start, quarter), columns]

    def quarters(h):
        return slice(h * quarter, (h + 1) * quarter)

    like = (xb.at[0, 0, 0 : rows // 2, 0:half], xb.at[0, 0, :, 0:half])
    spare = (0, 1, 2)
    a1 = [
        Scatter(
            links, place, "x", lambda d, h, j=j: z_part(d, j, h * quarter),
            a1s.at[j], a1r.at[j], like,
        )
        for j in range(N)
    ]
    a2 = Scatter(links, place, "z", lambda d, h: ra[d % N, quarters(h), :], a2s, a2r, like, spare)
    b1 = [
        Scatter(
            links, place, "z",
            lambda d, h, k=k: z_part(k, d, rows // 2 + h * quarter),
            b1s.at[k], b1r.at[k], like,
        )
        for k in range(N)
    ]
    b2 = Scatter(links, place, "x", lambda d, h: rb[d % N, quarters(h), :], b2s, b2r, like, spare)

    def dw_part(d, h):
        r = slice(d % N * pad, (d % N + 1) * pad)
        c = slice(h * half, (h + 1) * half)
        return dwf[r, c] + dwr[r, c].astype(F32)

    like_w = (wb.at[0, 0:pad], wb.at[0, 0 : 2 * pad])
    w1 = Scatter(links, place, "y", dw_part, ws, wr, like_w)
    order = (2, 1, 3, 0)

    def end(stage, out, k):
        for h, total in enumerate(stage[k % N].totals()):
            out[k % N, quarters(h), :] = total

    tx.after1()
    ty.after1()
    tx.forward1()
    tx.spread1()
    ty.spread1()
    wg.after()
    wg.after_rest()
    wu.after()
    wd.start()
    tx.after_f1()
    ty.forward1()
    tx.after2(0)
    ty.after2(0)
    wu.after_rest()
    wg.after_f()
    tx.after2(-1)
    ty.after2(-1)
    wu.after_f()
    wg.finish()
    wu.finish()
    forward(0, 1)
    tx.after2(1)
    ty.after2(1)
    wd.after()
    tx.after2_opposite()
    tx.after2_rest()
    wd.after_rest()
    forward(1, 1)
    ty.after_f1()
    wd.after_f()
    forward(-1, 1)
    wd.finish()
    ty.after_f2(-1)
    backward(-1)
    ty.after2_opposite()
    ty.after_f2(1)
    backward(1)
    for j in order:
        a1[j].direct_left()
        a1[j].direct_right()
    for k in (3, 1):
        b1[k].first()
    for k in (3, 1):
        b1[k].direct_right()
        b1[k].direct_left()
    ty.after_f2(0)
    tx.after_f2(0)
    tx.after_f2(-1)
    tx.after_f2(1)
    tx.after_f2(2)
    forward(2, 1)
    ty.after2_rest()
    ty.after_f2(2)
    backward(2)
    for j in order:
        a1[j].first()
    b1[2].first()
    b1[2].direct_right()
    b1[2].direct_left()
    backward(0)
    b1[3].second()
    b1[1].second()

    whole = xb[...].reshape(N * block, width)
    other = hidden // 2
    upper = slice(other // 2, other)
    lower = slice(0, other // 2)
    crossings = []

    def other_rows(part):
        pl.delay(1)
        wcs[part] = dot(dgate[other + part.start : other + part.stop], whole, (1, 0)).astype(BF16)
        crossings.append(links.group())
        links.copy(wcs.at[part], dwr.at[part], place.to("c", 1), crossings[-1], (1,))
        pl.delay(1)

    def own_rows(part):
        pl.delay(1)
        dwf[part] = dot(dgate[part], whole, (1, 0))
        pl.delay(1)

    other_rows(upper)
    own_rows(upper)
    b1[2].second()
    a1[2].second()
    a1[1].second()
    b1[0].first()
    other_rows(lower)
    crossings[0].wait(dwr.at[upper])
    w1.first()
    a1[3].second()
    own_rows(lower)
    a1[0].second()
    end(b1, rb, 2)
    b2.first()
    crossings[1].wait(dwr.at[lower])
    w1.direct_right()
    w1.direct_left()
    end(a1, ra, 2)
    a2.first()
    b1[0].second()
    b1[0].direct_right()
    b1[0].direct_left()
    end(b1, rb, 3)
    end(b1, rb, 1)
    end(a1, ra, 1)
    a2.direct_right()
    end(a1, ra, 3)
    a2.direct_left()
    b2.direct_left()
    b2.direct_right()
    w1.second()
    b2.second()
    a2.second()
    end(a1, ra, 0)
    end(b1, rb, 0)
    for h, total in enumerate(b2.totals()):
        dx_out[quarters(2 + h), :] = total.astype(BF16)
    for h, total in enumerate(a2.totals()):
        dx_out[quarters(h), :] = total.astype(BF16)
    for h, total in enumerate(w1.totals()):
        dw_out[:, h * half : (h + 1) * half] = total[0:units].astype(BF16)
    links.drain((dx, dx, xb))


def per_device(inputs, cotangent, gate_weight, up_weight, down_weight):
    rows, half = inputs.shape
    units, width = gate_weight.shape
    pad = -(-units // 16) * 16
    hidden = 2 * N * pad
    tokens = 2 * N * rows
    quarter = rows // 4
    vmem = pltpu.VMEM
    ring = (3, 2, quarter, half)
    scratch = [
        vmem((N, 2, rows, width), BF16),
        vmem((N, 2, rows, width), BF16),
        vmem((3, hidden, width), BF16),
        vmem((3, units, width), BF16),
        vmem((N, 2 * rows, 2 * hidden), F32),
        vmem((2 * rows, 2 * hidden), BF16),
        vmem((hidden, tokens), BF16),
        vmem((N, 2, rows, width), F32),
        vmem((N, rows // 2, half), F32),
        vmem((N, rows // 2, half), F32),
        vmem((hidden // 2, width), F32),
        vmem((hidden // 2, width), BF16),
        vmem((N,) + ring, BF16),
        vmem((N,) + ring, BF16),
        vmem(ring, BF16),
        vmem(ring, BF16),
        vmem((N,) + ring, BF16),
        vmem((N,) + ring, BF16),
        vmem(ring, BF16),
        vmem(ring, BF16),
        vmem((3, 2, pad, half), BF16),
        vmem((3, 2, pad, half), BF16),
        vmem((hidden // 2, width), BF16),
        pltpu.SemaphoreType.DMA((3,)),
        pltpu.SemaphoreType.DMA((GROUPS,)),
        pltpu.SemaphoreType.DMA((5,)),
    ]
    return pl.pallas_call(
        kernel,
        out_shape=(
            vmem((rows, half), BF16),
            vmem((units, width), BF16),
        ),
        in_specs=[pl.BlockSpec(memory_space=pltpu.HBM)] * 5,
        out_specs=(pl.BlockSpec(memory_space=vmem),) * 2,
        scratch_shapes=scratch,
        compiler_params=pltpu.CompilerParams(
            collective_id=0, has_side_effects=True, vmem_limit_bytes=VMEM_LIMIT
        ),
        name="swiglu_grads",
    )(inputs, cotangent, gate_weight, up_weight, down_weight)


def solution(mesh):
    torus = Mesh(
        mesh.devices.reshape(2, 4, 4, 2, mesh.shape["mp"]), ("dp_0", "dp_1", "dp_2", "dp_3", "mp")
    )
    return jax.shard_map(
        per_device,
        mesh=torus,
        in_specs=(P(DP, "mp"), P(DP, "mp"), P(MP_DP, None), P(MP_DP, None), P(MP_DP, None)),
        out_specs=(P(DP, "mp"), P(MP_DP, None)),
        check_vma=False,
    )
```

```python
import math

import jax
import jax.numpy as jnp
from jax import lax
from jax.experimental import pallas as pl
from jax.experimental.pallas import tpu as pltpu
from jax.sharding import Mesh
from jax.sharding import PartitionSpec as P

DP = ("dp_0", "dp_1", "dp_2", "dp_3")
MP_DP = ("mp", "dp_0", "dp_1", "dp_2", "dp_3")
MESH = pl.DeviceIdType.MESH
F32 = jnp.float32
BF16 = jnp.bfloat16
N = 4
GROUPS = 58
VMEM_LIMIT = 65000000
SLOT = (0, 1, 3, 2)


def dot(left, right, contract):
    return lax.dot_general(
        left, right, ((contract[:1], contract[1:]), ((), ())), preferred_element_type=F32
    )


class Group:
    def __init__(self, sem):
        self.sem = sem

    def wait(self, like):
        pltpu.make_async_copy(like, like, self.sem).wait()


class Links:
    def __init__(self, send, recv, limits):
        self.send, self.recv, self.limits = send, recv, limits
        self.groups = 0
        self.sent = [0] * len(limits)

    def group(self):
        self.groups += 1
        return Group(self.recv.at[self.groups - 1])

    def copy(self, src, dst, device, group, kinds=(0,)):
        size = math.prod(src.shape) * src.dtype.itemsize
        kind = next(k for k in kinds if self.sent[k] + size <= self.limits[k])
        self.sent[kind] += size
        pltpu.make_async_remote_copy(
            src_ref=src,
            dst_ref=dst,
            send_sem=self.send.at[kind],
            recv_sem=group.sem,
            device_id=device,
            device_id_type=MESH,
        ).start()

    def drain(self, refs):
        assert self.sent == self.limits, self.sent
        for k, ref in enumerate(refs):
            pltpu.make_async_copy(ref, ref, self.send.at[k]).wait()


class Place:
    def __init__(self):
        self.x = lax.axis_index("dp_1")
        self.y = lax.axis_index("dp_2")
        self.c = lax.axis_index("dp_3")
        self.z = lax.axis_index("dp_0") * 2 + lax.axis_index("mp")

    def at_z(self, dz):
        z = lax.rem(self.z + (dz + N), N)
        return lax.div(z, 2), lax.rem(z, 2)

    def to(self, axis, step):
        if axis == "x":
            return {"dp_1": lax.rem(self.x + (step + N), N)}
        if axis == "y":
            return {"dp_2": lax.rem(self.y + (step + N), N)}
        if axis == "z":
            high, low = self.at_z(step)
            return {"dp_0": high, "mp": low}
        return {"dp_3": 1 - self.c}


class Tokens:
    def __init__(self, links, place, buf, half, p, q):
        self.links, self.place, self.buf, self.half = links, place, buf, half
        self.p, self.q = p, q
        self.rows = buf.shape[2]
        self.s2, self.f2 = {}, {}

    def slot(self, dx, dz, h):
        high, low = self.place.at_z(dz)
        rows = pl.ds(0, self.rows) if h is None else pl.ds(h * self.rows // 2, self.rows // 2)
        columns = pl.ds(pl.multiple_of(low * self.half, 128), self.half)
        return self.buf.at[SLOT[dx % N], high, rows, columns]

    def piece(self, kp, kq):
        return (kp, kq) if self.p == "x" else (kq, kp)

    def push(self, kp, kq, h, axis, step, group):
        dx, dz = self.piece(kp, kq)
        ex = step if axis == "x" else 0
        self.links.copy(
            self.slot(dx, dz, h), self.slot(dx - ex, dz, h), self.place.to(axis, step), group
        )

    def pair(self, kp, kq, h, axis):
        group = self.links.group()
        for e in (1, -1):
            self.push(kp, kq, h, axis, e, group)
        return group

    def onward(self, pieces, axis):
        group = self.links.group()
        for (kp, kq), h, e in zip(pieces, (0, 1), (1, -1)):
            self.push(kp, kq, h, axis, e, group)
        return group

    def one(self):
        return self.buf.at[0, 0, :, 0 : self.half]

    def two(self):
        return self.buf.at[0, 0]

    def start1(self):
        self.s1 = self.pair(0, 0, None, self.p)

    def start2(self):
        self.s2[0] = self.pair(0, 0, None, self.q)

    def after1(self):
        self.s1.wait(self.two())

    def forward1(self):
        self.f1 = self.onward(((-1, 0), (1, 0)), self.p)

    def spread1(self):
        self.s2[-1] = self.pair(-1, 0, None, self.q)
        self.s2[1] = self.pair(1, 0, None, self.q)

    def after_f1(self):
        self.f1.wait(self.one())
        self.near = self.onward(((2, 0), (2, 0)), self.q)
        self.far = self.links.group()
        self.push(2, 0, 1, self.q, 1, self.far)
        self.push(2, 0, 0, self.q, -1, self.far)

    def after2(self, k):
        self.s2[k].wait(self.two())
        self.f2[k] = self.onward(((k, -1), (k, 1)), self.q)

    def after2_opposite(self):
        self.near.wait(self.one())
        self.f2[2] = self.onward(((2, -1), (2, 1)), self.q)

    def after2_rest(self):
        self.far.wait(self.one())

    def after_f2(self, k):
        self.f2[k].wait(self.one())


class Weight:
    def __init__(self, links, place, buf, pad):
        self.links, self.place, self.buf, self.pad = links, place, buf, pad
        self.width = buf.shape[1]

    def slot(self, c, dy, h):
        rows = pl.ds((c * N + dy % N) * self.pad, self.pad)
        if h is None:
            return self.buf.at[rows, :]
        return self.buf.at[rows, pl.ds(h * self.width // 2, self.width // 2)]

    def cross(self, dy):
        self.links.copy(
            self.slot(0, dy, None), self.slot(1, dy, None), self.place.to("c", 1), self.core, (1,)
        )

    def turn(self, dy, h, step, group):
        self.links.copy(
            self.slot(0, dy, h), self.slot(0, dy - step, h), self.place.to("y", step), group, (1,)
        )

    def one(self):
        return self.buf.at[0 : self.pad]

    def start(self):
        self.near, self.far, self.core = (self.links.group() for _ in range(3))
        self.turn(0, 0, 1, self.near)
        self.turn(0, 1, -1, self.near)
        self.turn(0, 1, 1, self.far)
        self.turn(0, 0, -1, self.far)
        self.cross(0)

    def after(self):
        self.near.wait(self.one())
        self.last = self.links.group()
        self.turn(-1, 0, 1, self.last)
        self.turn(1, 1, -1, self.last)

    def after_rest(self):
        self.far.wait(self.one())
        self.cross(-1)
        self.cross(1)

    def after_f(self):
        self.last.wait(self.one())
        self.cross(2)

    def finish(self):
        self.core.wait(self.buf.at[0 : N * self.pad])


class Scatter:
    def __init__(self, links, place, axis, mine, send, recv, like, kinds=(2,)):
        self.kinds = kinds
        self.links, self.place, self.axis = links, place, axis
        self.mine, self.send, self.recv, self.like = mine, send, recv, like
        self.early, self.late = links.group(), links.group()

    def go(self, value, u, h, step, group):
        self.send[u, h] = value.astype(BF16)
        self.links.copy(
            self.send.at[u, h], self.recv.at[u, h], self.place.to(self.axis, step), group,
            self.kinds,
        )

    def first(self):
        self.go(self.mine(2, 0), 0, 0, 1, self.early)
        self.go(self.mine(2, 1), 0, 1, -1, self.early)

    def direct_right(self):
        self.go(self.mine(1, 1), 1, 1, 1, self.late)

    def direct_left(self):
        self.go(self.mine(-1, 0), 2, 0, -1, self.late)

    def second(self):
        self.early.wait(self.like[0])
        self.go(self.mine(1, 0) + self.recv[0, 0].astype(F32), 1, 0, 1, self.late)
        self.go(self.mine(-1, 1) + self.recv[0, 1].astype(F32), 2, 1, -1, self.late)

    def totals(self):
        self.late.wait(self.like[1])
        return [
            self.mine(0, h) + self.recv[1, h].astype(F32) + self.recv[2, h].astype(F32)
            for h in range(2)
        ]


def kernel(
    x_ref, y_ref, g_ref, u_ref, d_ref, dx_out, dw_out,
    xb, yb, wb, win, gu, dgu, dgate, dx, ra, rb, dwf, dwr,
    a1s, a1r, a2s, a2r, b1s, b1r, b2s, b2r, ws, wr, wcs,
    send_sem, recv_sem, own_sem,
):
    place = Place()
    whole_bytes = math.prod(dx.shape) * 4
    links = Links(send_sem, recv_sem, [whole_bytes, whole_bytes, whole_bytes // 2])
    rows, half = x_ref.shape
    units, width = g_ref.shape
    hidden = wb.shape[1]
    pad = hidden // (2 * N)
    quarter = rows // 4
    block = 2 * rows

    barrier = pltpu.get_barrier_semaphore()
    peers = [("x", 1), ("x", -1), ("y", 1), ("y", -1), ("z", 1), ("z", -1), ("c", 1)]
    for axis, step in peers:
        pl.semaphore_signal(barrier, inc=1, device_id=place.to(axis, step), device_id_type=MESH)
    tx = Tokens(links, place, xb, half, "z", "x")
    ty = Tokens(links, place, yb, half, "x", "z")
    wg, wu, wd = (Weight(links, place, wb.at[m], pad) for m in range(3))
    pairs = [(x_ref, tx.slot(0, 0, None)), (y_ref, ty.slot(0, 0, None))]
    pairs += [(ref, win.at[m]) for m, ref in enumerate((g_ref, u_ref, d_ref))]
    loads = [pltpu.make_async_copy(a, b, own_sem.at[k]) for k, (a, b) in enumerate(pairs)]
    for c in loads:
        c.start()

    def place_weight(m):
        loads[2 + m].wait()
        if pad > units:
            low = units // 8 * 8
            wb[m, low:pad, :] = jnp.zeros((pad - low, width), BF16)
        wb[m, 0:units, :] = win[m]

    for c in loads[:2]:
        c.wait()
    pl.semaphore_wait(barrier, len(peers))
    tx.start1()
    ty.start1()
    tx.start2()
    ty.start2()
    place_weight(0)
    wg.start()
    place_weight(1)
    wu.start()
    place_weight(2)

    def spot(k):
        return SLOT[k % N]

    def forward(k, count):
        a = spot(k)
        pl.delay(1)
        tokens = xb[a : a + count].reshape(count * block, width)
        both = dot(tokens, wb[0:2].reshape(2 * hidden, width), (1, 1))
        gu[a : a + count] = both.reshape(count, block, 2 * hidden)
        pl.delay(1)

    def backward(k):
        a = spot(k)
        pl.delay(1)
        dh = dot(yb[a].reshape(block, width), wb[2], (1, 1))
        g = gu[a, :, 0:hidden]
        sig = jax.nn.sigmoid(g)
        dg = (dh * gu[a, :, hidden:] * sig * (1.0 + g * (1.0 - sig))).astype(BF16)
        dgu[:, 0:hidden] = dg
        dgu[:, hidden:] = (dh * (g * sig)).astype(BF16)
        part = dot(dgu[...], wb[0:2].reshape(2 * hidden, width), (1, 0))
        dx[a] = part.reshape(2, rows, width)
        dgate[:, a * block : (a + 1) * block] = dgu[:, 0:hidden].T
        pl.delay(1)

    def z_part(k, d, start):
        high, low = place.at_z(d)
        columns = pl.ds(pl.multiple_of(low * half, 128), half)
        return dx[spot(k), high, pl.ds(start, quarter), columns]

    def quarters(h):
        return slice(h * quarter, (h + 1) * quarter)

    like = (xb.at[0, 0, 0 : rows // 2, 0:half], xb.at[0, 0, :, 0:half])
    spare = (0, 1, 2)
    a1 = [
        Scatter(
            links, place, "x", lambda d, h, j=j: z_part(d, j, h * quarter),
            a1s.at[j], a1r.at[j], like,
        )
        for j in range(N)
    ]
    a2 = Scatter(links, place, "z", lambda d, h: ra[d % N, quarters(h), :], a2s, a2r, like, spare)
    b1 = [
        Scatter(
            links, place, "z",
            lambda d, h, k=k: z_part(k, d, rows // 2 + h * quarter),
            b1s.at[k], b1r.at[k], like,
        )
        for k in range(N)
    ]
    b2 = Scatter(links, place, "x", lambda d, h: rb[d % N, quarters(h), :], b2s, b2r, like, spare)

    def dw_part(d, h):
        r = slice(d % N * pad, (d % N + 1) * pad)
        c = slice(h * half, (h + 1) * half)
        return dwf[r, c] + dwr[r, c].astype(F32)

    like_w = (wb.at[0, 0:pad], wb.at[0, 0 : 2 * pad])
    w1 = Scatter(links, place, "y", dw_part, ws, wr, like_w)
    order = (2, 1, 3, 0)

    def end(stage, out, k):
        for h, total in enumerate(stage[k % N].totals()):
            out[k % N, quarters(h), :] = total

    tx.after1()
    ty.after1()
    tx.forward1()
    tx.spread1()
    ty.spread1()
    wg.after()
    wg.after_rest()
    wu.after()
    wd.start()
    tx.after_f1()
    ty.forward1()
    tx.after2(0)
    ty.after2(0)
    wu.after_rest()
    wg.after_f()
    tx.after2(-1)
    ty.after2(-1)
    wu.after_f()
    wg.finish()
    wu.finish()
    forward(0, 1)
    tx.after2(1)
    ty.after2(1)
    wd.after()
    tx.after2_opposite()
    tx.after2_rest()
    wd.after_rest()
    forward(1, 1)
    ty.after_f1()
    wd.after_f()
    forward(-1, 1)
    wd.finish()
    ty.after_f2(-1)
    backward(-1)
    ty.after2_opposite()
    ty.after_f2(1)
    backward(1)
    for j in order:
        a1[j].direct_left()
        a1[j].direct_right()
    for k in (3, 1):
        b1[k].first()
    for k in (3, 1):
        b1[k].direct_right()
        b1[k].direct_left()
    ty.after_f2(0)
    tx.after_f2(0)
    tx.after_f2(-1)
    tx.after_f2(1)
    tx.after_f2(2)
    forward(2, 1)
    ty.after2_rest()
    ty.after_f2(2)
    backward(2)
    for j in order:
        a1[j].first()
    b1[2].first()
    b1[2].direct_right()
    b1[2].direct_left()
    backward(0)
    b1[3].second()
    b1[1].second()

    whole = xb[...].reshape(N * block, width)
    other = hidden // 2
    upper = slice(other // 2, other)
    lower = slice(0, other // 2)
    crossings = []

    def other_rows(part):
        pl.delay(1)
        wcs[part] = dot(dgate[other + part.start : other + part.stop], whole, (1, 0)).astype(BF16)
        crossings.append(links.group())
        links.copy(wcs.at[part], dwr.at[part], place.to("c", 1), crossings[-1], (1,))
        pl.delay(1)

    def own_rows(part):
        pl.delay(1)
        dwf[part] = dot(dgate[part], whole, (1, 0))
        pl.delay(1)

    other_rows(upper)
    own_rows(upper)
    b1[2].second()
    a1[2].second()
    a1[1].second()
    b1[0].first()
    other_rows(lower)
    crossings[0].wait(dwr.at[upper])
    w1.first()
    a1[3].second()
    own_rows(lower)
    end(b1, rb, 2)
    b2.first()
    a1[0].second()
    crossings[1].wait(dwr.at[lower])
    w1.direct_right()
    w1.direct_left()
    end(a1, ra, 2)
    a2.first()
    b1[0].second()
    b1[0].direct_right()
    b1[0].direct_left()
    end(b1, rb, 3)
    end(b1, rb, 1)
    end(a1, ra, 1)
    a2.direct_right()
    end(a1, ra, 3)
    a2.direct_left()
    b2.direct_left()
    b2.direct_right()
    w1.second()
    b2.second()
    a2.second()
    end(a1, ra, 0)
    end(b1, rb, 0)
    for h, total in enumerate(b2.totals()):
        dx_out[quarters(2 + h), :] = total.astype(BF16)
    for h, total in enumerate(a2.totals()):
        dx_out[quarters(h), :] = total.astype(BF16)
    for h, total in enumerate(w1.totals()):
        dw_out[:, h * half : (h + 1) * half] = total[0:units].astype(BF16)
    links.drain((dx, dx, xb))


def per_device(inputs, cotangent, gate_weight, up_weight, down_weight):
    rows, half = inputs.shape
    units, width = gate_weight.shape
    pad = -(-units // 16) * 16
    hidden = 2 * N * pad
    tokens = 2 * N * rows
    quarter = rows // 4
    vmem = pltpu.VMEM
    ring = (3, 2, quarter, half)
    scratch = [
        vmem((N, 2, rows, width), BF16),
        vmem((N, 2, rows, width), BF16),
        vmem((3, hidden, width), BF16),
        vmem((3, units, width), BF16),
        vmem((N, 2 * rows, 2 * hidden), F32),
        vmem((2 * rows, 2 * hidden), BF16),
        vmem((hidden, tokens), BF16),
        vmem((N, 2, rows, width), F32),
        vmem((N, rows // 2, half), F32),
        vmem((N, rows // 2, half), F32),
        vmem((hidden // 2, width), F32),
        vmem((hidden // 2, width), BF16),
        vmem((N,) + ring, BF16),
        vmem((N,) + ring, BF16),
        vmem(ring, BF16),
        vmem(ring, BF16),
        vmem((N,) + ring, BF16),
        vmem((N,) + ring, BF16),
        vmem(ring, BF16),
        vmem(ring, BF16),
        vmem((3, 2, pad, half), BF16),
        vmem((3, 2, pad, half), BF16),
        vmem((hidden // 2, width), BF16),
        pltpu.SemaphoreType.DMA((3,)),
        pltpu.SemaphoreType.DMA((GROUPS,)),
        pltpu.SemaphoreType.DMA((5,)),
    ]
    return pl.pallas_call(
        kernel,
        out_shape=(
            vmem((rows, half), BF16),
            vmem((units, width), BF16),
        ),
        in_specs=[pl.BlockSpec(memory_space=pltpu.HBM)] * 5,
        out_specs=(pl.BlockSpec(memory_space=vmem),) * 2,
        scratch_shapes=scratch,
        compiler_params=pltpu.CompilerParams(
            collective_id=0, has_side_effects=True, vmem_limit_bytes=VMEM_LIMIT
        ),
        name="swiglu_grads",
    )(inputs, cotangent, gate_weight, up_weight, down_weight)


def solution(mesh):
    torus = Mesh(
        mesh.devices.reshape(2, 4, 4, 2, mesh.shape["mp"]), ("dp_0", "dp_1", "dp_2", "dp_3", "mp")
    )
    return jax.shard_map(
        per_device,
        mesh=torus,
        in_specs=(P(DP, "mp"), P(DP, "mp"), P(MP_DP, None), P(MP_DP, None), P(MP_DP, None)),
        out_specs=(P(DP, "mp"), P(MP_DP, None)),
        check_vma=False,
    )
```
